512 devices in a mesh: groups: 2 (over y), seq: 32 (over z, core), rep: 8 (over x).
Axes of the slice: x: 8, y: 2, z: 16, core: 2. Of those that a mesh axis runs over, the one named last changes fastest.
The devices are a block of a 8x16x16 slice.
Arguments:
- queries: bfloat16 [1024, 4096], P(('groups', 'seq'), 'rep'), parts along dimension 0, may hold values from -128 to 128
- keys_new: bfloat16 [1024, 1024], P(('groups', 'seq'), 'rep'), parts along dimension 0, may hold values from -4 to 4
- values_new: bfloat16 [1024, 1024], P(('groups', 'seq'), 'rep'), parts along dimension 0, may hold values from -6 to 6
- keys_past: bfloat16 [16384, 1024], P(('groups', 'seq'), 'rep'), parts along dimension 0, may hold values from -4 to 4
- values_past: bfloat16 [16384, 1024], P(('groups', 'seq'), 'rep'), parts along dimension 0, may hold values from -6 to 6
- block_order: int32 [64], P('groups'), parts along dimension 0, may hold values from 0 to 31, each once
- residual: bfloat16 [1024, 4096], P(('groups', 'seq'), 'rep'), parts along dimension 0, may hold values from -6 to 6
- out_proj: bfloat16 [4096, 4096], P('seq', 'rep'), may hold values from -0.09375 to 0.09375
- norm_gain: float32 [4096], replicated, may hold values from 0.5 to 1.5
- router: float32 [4096, 4], replicated, may hold values from -0.09375 to 0.09375
- w_gate: bfloat16 [8, 4096, 4096], P('rep', None, 'seq'), may hold values from -0.09375 to 0.09375
- w_up: bfloat16 [8, 4096, 4096], P('rep', None, 'seq'), may hold values from -0.09375 to 0.09375
- w_down: bfloat16 [8, 4096, 4096], P('rep', 'seq'), may hold values from -0.0625 to 0.0625
- expert_ids: int32 [1024, 2], P(('groups', 'seq')), parts along dimension 0, may hold values from 0 to 3, all different within a row; in each aligned block of 16 rows (0 to 15, 16 to 31, ...) at most 12 rows name the same one
Outputs:
- attended: bfloat16 [1024, 4096], P(('groups', 'seq'), 'rep'), parts along dimension 0
- layer_out: bfloat16 [1024, 4096], P(('groups', 'seq'), 'rep'), parts along dimension 0
- keys_cache: bfloat16 [1024, 1024], P(('groups', 'seq')), parts along dimension 0
- values_cache: bfloat16 [1024, 1024], P(('groups', 'seq')), parts along dimension 0
The draws below stay inside these ranges and needn't reach their ends.
There are 2 independent parts, one for each index of `groups`. The reference program is written for one: setup_inputs(seed, part) draws one part's arguments, and reference() takes and returns one part's arrays. A program takes and returns all parts, laid end to end along the dimension named above; an argument that names none is the same for every part. Nothing has to cross between parts.
Inputs may be any that keep to these rules, and one draw needn't show every extreme that they name: `block_order`: each block index 0 to 32 - 1 appears once. `expert_ids`: each row names 2 different experts; in the rows of one device (aligned blocks of 16 rows) no expert is named by more than 12 rows, and in some block one expert is named by exactly 12.
All inputs are finite; a program needn't handle non-finite values.
Results may differ from the reference program's by a relative error of at most 0.011.
Values may be sent and summed in bfloat16 or wider, within the bound.
No kernel may reach another device: no remote copies, remote signals or barrier semaphores. Data moves between devices by JAX's collectives and lax.ppermute only.
A program may use at most 64 MiB of HBM per device.

```python
import math
import jax
import jax.numpy as jnp
import numpy as np
from jax import lax

D = 4096
HD = 128
Q_PER = 4
KV_HEADS = 8
HEADS = 32
EXPERTS = 4
TOP = 2
FF = 8192
TOK_DEV = 16
CAP = 12
HALVES = 2
S_NEW = 512
CTX = 8192
N_SEQ = 32


def drawn_pair(key):
    base = jax.random.fold_in(key, 11)
    key_seed, query_seed = jax.random.split(base)
    past_keys = jnp.clip(jax.random.normal(key_seed, (CTX, KV_HEADS * HD), jnp.float32), -4.0, 4.0)
    query_rows = jnp.clip(jax.random.normal(query_seed, (S_NEW, KV_HEADS * Q_PER * HD), jnp.float32), -4.0, 4.0)
    return (past_keys, query_rows)


def draw_queries(key, part):
    past_keys, query_rows = drawn_pair(key)
    return query_rows.astype(jnp.bfloat16)


def draw_keys_past(key, part):
    past_keys, query_rows = drawn_pair(key)
    return past_keys.astype(jnp.bfloat16)


def block_levels(own_key, shape, cuts, least, high):
    def one(dim, shards_of):
        draws = jax.random.uniform(jax.random.fold_in(jax.random.fold_in(own_key, 6), dim), (shards_of,), jnp.float32, least / len(cuts), high / len(cuts))
        return jnp.repeat(jnp.exp(draws), shape[dim] // shards_of).reshape((-1,) + (1,) * (len(shape) - dim - 1))

    loudness = one(*cuts[0])
    for cut in cuts[1:]:
        loudness = loudness * one(*cut)
    return loudness


def routed_block(key, own, number, rows, count, top, bound, lean):
    sequence = jax.random.permutation(key, count)
    heavy_load, usual = portions_of(count, rows * top, bound, lean, True), portions_of(count, rows * top, bound, lean, False)
    places = jnp.arange(count)

    def named(tallies, turn):
        used = int((tallies > 0).sum())
        fixed = max(1, used // 4)
        passed = fixed + (places - fixed + turn * (used - fixed)) % max(1, count - fixed)
        return jnp.zeros((count,), jnp.int32).at[sequence[jnp.where(places < fixed, places, passed)]].set(jnp.asarray(tallies, jnp.int32))

    tallies = jnp.where(number % 4 == 0, named(heavy_load, number // 4), named(usual, number - number // 4 - 1))
    mixed = jax.random.permutation(jax.random.fold_in(own, 3), count)
    giver, taker = mixed[0:count // 2 * 2:2], mixed[1:count // 2 * 2:2]
    room = jnp.minimum(tallies[giver] - 1, bound - tallies[taker]) // 2
    room = jnp.where((giver == sequence[0]) | (taker == sequence[0]) | (tallies[taker] == 0), 0, jnp.maximum(room, 0))
    passed = jax.random.randint(jax.random.fold_in(own, 4), (count // 2,), 0, 1 << 20) % (room + 1)
    tallies = tallies.at[giver].add(-passed).at[taker].add(passed)
    labels = jnp.searchsorted(jnp.cumsum(tallies), jnp.arange(rows * top), side="right").astype(jnp.int32)
    table = labels.reshape(top, rows).T
    table = table[jax.random.permutation(jax.random.fold_in(own, 1), rows)]
    turn = jax.random.randint(jax.random.fold_in(own, 2), (rows, 1), 0, top)
    return jnp.take_along_axis(table, (jnp.arange(top)[None, :] + turn) % top, axis=1)


def portions_of(amount, total, most, skew, full):
    loads = [(1 << 20) // math.isqrt(grade ** skew) + 1 for grade in range(1, amount + 1)]
    largest = most if full else min(most, max(-(-total // amount), total * loads[0] // sum(loads)))
    least = 1 if total - largest >= amount - 1 else 0
    given, spare = [largest] + [least] * (amount - 1), total - largest - least * (amount - 1)
    while spare > 0:
        movable = [i for i in range(1, amount) if given[i] < largest] or [i for i in range(1, amount) if given[i] < most]
        mass, remaining = sum([loads[i] for i in movable]), spare
        for i in movable:
            addition = min(most - given[i], max(1, remaining * loads[i] // mass), spare)
            given[i] = given[i] + addition
            spare = spare - addition
    return np.array(given)


def noise(stream_key, shape, scale, reach, cuts=(), kind=jnp.bfloat16):
    level = block_levels(stream_key, shape, cuts, -0.22, 0.18) if cuts else 1.0
    values = jax.random.normal(stream_key, shape, jnp.float32) * scale * level
    return jnp.minimum(jnp.maximum(values, -reach), reach).astype(kind)


def setup_inputs(seed: int = 0, part: int = 0) -> dict:
    streams_of = jax.random.split(jax.random.key(seed), 15)
    part_keys = jax.random.split(jax.random.fold_in(streams_of[14], part), 15)
    queries = draw_queries(jax.random.fold_in(jax.random.fold_in(streams_of[14], part), 71), part)
    keys_new = noise(part_keys[1], (S_NEW, KV_HEADS * HD), 1.0, 4.0, ((0, 32), (1, 8)))
    values_new = noise(part_keys[2], (S_NEW, KV_HEADS * HD), 1.0, 6.0, ((0, 32), (1, 8)))
    keys_past = draw_keys_past(jax.random.fold_in(jax.random.fold_in(streams_of[14], part), 71), part)
    values_past = noise(part_keys[4], (CTX, KV_HEADS * HD), 1.0, 6.0, ((0, 32), (1, 8)))
    block_order = jax.random.permutation(part_keys[5], N_SEQ).astype(jnp.int32)
    residual = noise(part_keys[6], (S_NEW, D), 1.0, 6.0, ((0, 32), (1, 8)))
    out_proj = noise(streams_of[7], (HEADS * HD, D), (HEADS * HD) ** -0.5, 0.09375, ((0, 32), (1, 8)))
    norm_gain = jnp.clip(1.0 + 0.1 * jax.random.normal(streams_of[8], (D,), jnp.float32), 0.5, 1.5)
    router = noise(streams_of[9], (D, EXPERTS), D ** -0.5, 0.09375, (), jnp.float32)
    w_gate = noise(streams_of[10], (EXPERTS * HALVES, D, FF // HALVES), D ** -0.5, 0.09375, ((0, 8), (2, 32)))
    w_up = noise(streams_of[11], (EXPERTS * HALVES, D, FF // HALVES), D ** -0.5, 0.09375, ((0, 8), (2, 32)))
    w_down = noise(streams_of[12], (EXPERTS * HALVES, FF // HALVES, D), FF ** -0.5, 0.0625, ((0, 8), (1, 32)))
    expert_ids_keys = jax.random.split(jax.random.fold_in(part_keys[13], 1), S_NEW // TOK_DEV)
    expert_ids_turns = jax.random.permutation(jax.random.fold_in(part_keys[13], 3), S_NEW // TOK_DEV)
    expert_ids = jax.vmap(lambda own, number: routed_block(jax.random.fold_in(part_keys[13], 2), own, number, TOK_DEV, EXPERTS, TOP, CAP, 2))(expert_ids_keys, expert_ids_turns).reshape((S_NEW, TOP))
    return {"queries": queries, "keys_new": keys_new, "values_new": values_new, "keys_past": keys_past, "values_past": values_past, "block_order": block_order, "residual": residual, "out_proj": out_proj, "norm_gain": norm_gain, "router": router, "w_gate": w_gate, "w_up": w_up, "w_down": w_down, "expert_ids": expert_ids}


def reference(queries, keys_new, values_new, keys_past, values_past, block_order, residual, out_proj, norm_gain, router, w_gate, w_up, w_down, expert_ids):
    token_index = jnp.arange(S_NEW, dtype=jnp.int32)
    position = block_order[token_index // TOK_DEV] * TOK_DEV + token_index % TOK_DEV
    new_visible = position[None, :] <= position[:, None]
    row_visible = jnp.concatenate([jnp.ones((S_NEW, CTX), dtype=bool), new_visible], axis=1)
    row_visible = jnp.repeat(row_visible, Q_PER, axis=0)
    query_heads = queries.reshape(S_NEW, KV_HEADS, Q_PER, HD).transpose(1, 0, 2, 3).reshape(KV_HEADS, S_NEW * Q_PER, HD)
    keys_all = jnp.concatenate([keys_past, keys_new], axis=0).reshape(CTX + S_NEW, KV_HEADS, HD).transpose(1, 0, 2)
    values_all = jnp.concatenate([values_past, values_new], axis=0).reshape(CTX + S_NEW, KV_HEADS, HD).transpose(1, 0, 2)

    def one_head(operands):
        query_block, key_block, value_block = operands
        scores = jnp.dot(query_block, key_block.T, preferred_element_type=jnp.float32) * (1.0 / math.sqrt(HD))
        highest = lax.optimization_barrier(jnp.max(jnp.where(row_visible, scores, -jnp.inf), axis=1, keepdims=True))
        weights = jnp.where(row_visible, jnp.exp(scores - highest), 0.0)
        numerator = jnp.dot(weights.astype(jnp.bfloat16), value_block, preferred_element_type=jnp.float32)
        return (numerator / lax.optimization_barrier(jnp.sum(weights, axis=1, keepdims=True))).astype(jnp.bfloat16)
    heads_out = lax.map(one_head, (query_heads, keys_all, values_all))
    attended_heads = heads_out.reshape(KV_HEADS, S_NEW, Q_PER * HD).transpose(1, 0, 2).reshape(S_NEW, KV_HEADS * Q_PER * HD)
    projected = jnp.dot(attended_heads, out_proj, preferred_element_type=jnp.float32)
    attended = (residual.astype(jnp.float32) + projected).astype(jnp.bfloat16)
    features = attended.astype(jnp.float32)
    mean_square = lax.optimization_barrier(jnp.mean(features * features, axis=1, keepdims=True))
    normed = (features * norm_gain[None, :] * lax.rsqrt(mean_square + 1e-05)).astype(jnp.bfloat16)
    logits = jnp.dot(normed.astype(jnp.float32), router, precision=lax.Precision.HIGHEST)
    expert_range = jnp.arange(EXPERTS, dtype=jnp.int32)
    first_pick = (expert_ids[:, 0:1] == expert_range[None, :]).astype(jnp.float32)
    second_pick = (expert_ids[:, 1:2] == expert_range[None, :]).astype(jnp.float32)
    share_first = jax.nn.sigmoid(lax.optimization_barrier(jnp.sum(first_pick * logits, axis=1)) - lax.optimization_barrier(jnp.sum(second_pick * logits, axis=1)))
    token_share = share_first[:, None] * first_pick + (1.0 - share_first)[:, None] * second_pick
    block_count = HALVES * N_SEQ
    block_width = FF // block_count
    mixture = jnp.zeros((S_NEW, D), jnp.float32)

    def add_block(running_sum, operands):
        act_piece, down_piece = operands
        partial_sum = jnp.dot(act_piece, down_piece, preferred_element_type=jnp.float32)
        rounded = lax.optimization_barrier(partial_sum.astype(jnp.bfloat16))
        return (running_sum + rounded.astype(jnp.float32), None)
    for expert in range(EXPERTS):
        gate_full = jnp.concatenate([w_gate[half_index * EXPERTS + expert] for half_index in range(HALVES)], axis=1)
        up_full = jnp.concatenate([w_up[half_index * EXPERTS + expert] for half_index in range(HALVES)], axis=1)
        down_full = jnp.concatenate([w_down[half_index * EXPERTS + expert] for half_index in range(HALVES)], axis=0)
        gate_part = jnp.dot(normed, gate_full, preferred_element_type=jnp.float32)
        up_part = jnp.dot(normed, up_full, preferred_element_type=jnp.float32)
        activation = (jax.nn.silu(gate_part) * up_part).astype(jnp.bfloat16)
        act_blocks = activation.reshape(S_NEW, block_count, block_width).transpose(1, 0, 2)
        down_blocks = down_full.reshape(block_count, block_width, D)
        expert_out, ignored = lax.scan(add_block, jnp.zeros((S_NEW, D), jnp.float32), (act_blocks, down_blocks))
        mixture = mixture + token_share[:, expert:expert + 1] * expert_out
    layer_out = (features + mixture).astype(jnp.bfloat16)
    return (attended, layer_out, keys_new, values_new)
```

```python
import math

import jax
import jax.numpy as jnp
from jax import lax
from jax.sharding import Mesh
from jax.sharding import PartitionSpec as P

EXPERTS = 4
CAP = 12
LANES = 128
PAIR = 2
CORES = 2
SEQ = ("far", "near", "core")
TOKENS = ("groups", "far", "near", "core")
ATT_SHARE = ("core",)
ATT_CLASS = ("far", "near")
MOE_SHARE = ("near", "core")
MOE_CLASS = ("far",)


def swapped(array, axis):
    return lax.ppermute(array, axis, [(0, 1), (1, 0)])


def shared_by(array, axes):
    held = [array]
    for axis in axes:
        held = held + [swapped(a, axis) for a in held]
    return held


def owners_by(axes):
    place = {a: lax.axis_index(a) for a in SEQ}
    held = [place]
    for axis in axes:
        held = held + [{**p, axis: 1 - p[axis]} for p in held]
    sizes = {a: lax.axis_size(a) for a in SEQ}
    return [(p["far"] * sizes["near"] + p["near"]) * sizes["core"] + p["core"] for p in held]


def exchanged(tiles, axis):
    return lax.all_to_all(tiles, axis, 0, 0, tiled=True)


def sent_to_all(array, axis):
    return exchanged(jnp.broadcast_to(array[None], (lax.axis_size(axis), *array.shape)), axis)


def side_by_side(tiles):
    return jnp.concatenate([tiles[i] for i in range(tiles.shape[0])], axis=1)


def block_lookup(owners, block_order):
    width = block_order.shape[0]
    hits = owners[:, None] == jnp.arange(width, dtype=jnp.int32)[None, :]
    return jnp.sum(jnp.where(hits, block_order[None, :], 0), axis=1)


def class_places(axes):
    sizes = {a: lax.axis_size(a) for a in SEQ}
    count = lax.axis_size(axes)
    index = jnp.arange(count, dtype=jnp.int32)
    place = {a: jnp.full((count,), lax.axis_index(a), jnp.int32) for a in SEQ}
    for axis in reversed(axes):
        place[axis] = index % sizes[axis]
        index = index // sizes[axis]
    return (place["far"] * sizes["near"] + place["near"]) * sizes["core"] + place["core"]


def body(
    queries,
    keys_new,
    values_new,
    keys_past,
    values_past,
    block_order,
    residual,
    out_proj,
    norm_gain,
    router,
    w_gate,
    w_up,
    w_down,
    expert_ids,
):
    bf16, f32 = jnp.bfloat16, jnp.float32
    tok = queries.shape[0]
    head_dim = keys_new.shape[1]
    q_per = queries.shape[1] // head_dim
    width = queries.shape[1]
    past_len = keys_past.shape[0]
    rep_count = lax.axis_size("rep")
    scaling = 1.0 / math.sqrt(head_dim)

    gate_up = jnp.concatenate([w_gate[0], w_up[0]], axis=1)
    gate_ups = shared_by(gate_up, MOE_SHARE)
    downs = shared_by(w_down[0], MOE_SHARE)
    kv_local = jnp.concatenate(
        [
            jnp.concatenate([keys_past, keys_new], axis=0),
            jnp.concatenate([values_past, values_new], axis=0),
        ],
        axis=1,
    )
    kv_all = jnp.concatenate(shared_by(kv_local, ATT_SHARE), axis=0)
    out_proj_all = lax.all_gather(out_proj, SEQ, axis=0, tiled=True)

    ids_wide = jnp.pad(expert_ids.astype(bf16), ((0, 0), (0, LANES - expert_ids.shape[1])))
    query_class = lax.all_gather(
        jnp.concatenate([queries, ids_wide], axis=1), ATT_CLASS, axis=0, tiled=True
    )
    att_count = lax.axis_size(ATT_CLASS)
    rows = att_count * tok
    ids_att = query_class[:, width : width + 2].astype(jnp.int32)
    query_pos = (
        block_lookup(class_places(ATT_CLASS), block_order)[:, None] * tok
        + jnp.arange(tok, dtype=jnp.int32)[None, :]
    ).reshape(rows)

    key_span = past_len + tok
    key_owner_pos = block_lookup(jnp.stack(owners_by(ATT_SHARE)), block_order)
    offset = jnp.arange(key_span, dtype=jnp.int32) - past_len
    key_pos = jnp.where(
        offset[None, :] >= 0, key_owner_pos[:, None] * tok + offset[None, :], -1
    ).reshape(-1)
    visible = key_pos[None, :] <= query_pos[:, None]
    keys, values = kv_all[:, :head_dim], kv_all[:, head_dim:]
    heads = jnp.stack(
        [query_class[:, j * head_dim : (j + 1) * head_dim] for j in range(q_per)], axis=0
    )
    scores = jnp.einsum("jtd,kd->jtk", heads, keys, preferred_element_type=f32) * scaling
    scores = jnp.where(visible[None], scores, -1e30)
    shift = jnp.max(scores, axis=2).astype(bf16)
    weights = jnp.exp(scores - shift.astype(f32)[:, :, None])
    totals = jnp.sum(weights, axis=2)
    partial = jnp.einsum("jtk,kd->jtd", weights.astype(bf16), values, preferred_element_type=f32)
    totals_high = totals.astype(bf16)
    totals_low = (totals - totals_high.astype(f32)).astype(bf16)
    notes = jnp.concatenate([shift, totals_high, totals_low], axis=0).T
    notes = jnp.pad(notes, ((0, 0), (0, LANES - notes.shape[1])))
    message = jnp.concatenate([partial[j].astype(bf16) for j in range(q_per)] + [notes], axis=1)
    parts = exchanged(message.reshape(att_count, tok, width + LANES), ATT_CLASS)
    part_shift = parts[:, :, width : width + q_per].astype(f32)
    part_total = parts[:, :, width + q_per : width + 2 * q_per].astype(f32) + parts[
        :, :, width + 2 * q_per : width + 3 * q_per
    ].astype(f32)
    level = jnp.exp(part_shift - jnp.max(part_shift, axis=0, keepdims=True))
    total = jnp.sum(level * part_total, axis=0)
    attn_local = jnp.concatenate(
        [
            jnp.sum(
                level[:, :, j : j + 1]
                * parts[:, :, j * head_dim : (j + 1) * head_dim].astype(f32),
                axis=0,
            )
            / total[:, j : j + 1]
            for j in range(q_per)
        ],
        axis=1,
    ).astype(bf16)

    spread = sent_to_all(jnp.concatenate([attn_local, keys_new, values_new], axis=1), "rep")
    attn_full = side_by_side(spread[:, :, :width])
    keys_cache = side_by_side(spread[:, :, width : width + head_dim])
    values_cache = side_by_side(spread[:, :, width + head_dim :])
    projected = jnp.dot(attn_full, out_proj_all, preferred_element_type=f32)
    attended = (residual.astype(f32) + projected).astype(bf16)

    moe_count = lax.axis_size(MOE_CLASS)
    class_rows = moe_count * tok
    class_width = attended.shape[1]
    class_attended = lax.all_gather(attended, MOE_CLASS, axis=0, tiled=True)
    ids = ids_att.reshape(att_count, tok, 2)
    if ATT_CLASS != MOE_CLASS:
        ids = lax.dynamic_index_in_dim(
            ids.reshape(moe_count, att_count // moe_count, tok, 2),
            lax.axis_index("near"),
            axis=1,
            keepdims=False,
        )
    ids = ids.reshape(class_rows, 2)
    experts = jnp.arange(EXPERTS, dtype=jnp.int32)
    first_pick = (ids[:, 0:1] == experts[None, :]).astype(f32)
    second_pick = (ids[:, 1:2] == experts[None, :]).astype(f32)
    member = first_pick + second_pick
    row = jnp.arange(class_rows, dtype=jnp.int32)
    earlier = (row[:, None] // tok == row[None, :] // tok) & (row[None, :] < row[:, None])
    ranking = jnp.dot(
        earlier.astype(bf16), member.astype(bf16), preferred_element_type=f32
    ).astype(jnp.int32)
    slot_of = jnp.where(member > 0, (row[:, None] // tok) * CAP + ranking, -1)
    slot_count = moe_count * CAP
    slots = jnp.arange(slot_count, dtype=jnp.int32)
    selection = (slot_of.T[:, None, :] == slots[None, :, None]).astype(bf16)
    slot_rows = jnp.dot(
        selection.reshape(EXPERTS * slot_count, class_rows),
        class_attended,
        preferred_element_type=f32,
    ).astype(bf16)
    slot_rows = slot_rows.reshape(EXPERTS, slot_count, class_width)
    halves = rep_count // EXPERTS
    arrived = exchanged(jnp.concatenate([slot_rows] * halves, axis=0), "rep")
    features = side_by_side(arrived).astype(f32)

    mean_square = jnp.mean(features * features, axis=1, keepdims=True)
    normed = (features * norm_gain[None, :] * lax.rsqrt(mean_square + 1e-05)).astype(bf16)
    logits = jnp.dot(normed.astype(f32), router, precision=lax.Precision.HIGHEST)
    mine = lax.axis_index("rep") % EXPERTS
    my_selection = lax.dynamic_index_in_dim(selection, mine, axis=0, keepdims=False)
    slot_member = jnp.dot(my_selection, member.astype(bf16), preferred_element_type=f32)
    own = (experts == mine)[None, :]
    own_logit = jnp.sum(jnp.where(own, logits, 0.0), axis=1)
    other_logit = jnp.sum(jnp.where(own, 0.0, slot_member * logits), axis=1)
    share = jax.nn.sigmoid(own_logit - other_logit)
    hidden_width = w_gate.shape[2]
    expert_out = None
    for gu, down in zip(gate_ups, downs):
        both = jnp.dot(normed, gu, preferred_element_type=f32)
        hidden = (jax.nn.silu(both[:, :hidden_width]) * both[:, hidden_width:]).astype(bf16)
        piece = jnp.dot(hidden, down, preferred_element_type=f32)
        expert_out = piece if expert_out is None else expert_out + piece
    weighted = (expert_out * share[:, None]).astype(bf16)
    outgoing = jnp.stack(
        [weighted[:, i * class_width : (i + 1) * class_width] for i in range(rep_count)], axis=0
    )
    returned = exchanged(outgoing, "rep")

    back = jnp.concatenate([selection.reshape(EXPERTS * slot_count, class_rows)] * halves, axis=0)
    mixture = lax.dot_general(
        back,
        returned.reshape(rep_count * slot_count, class_width),
        (((0,), (0,)), ((), ())),
        preferred_element_type=f32,
    ).astype(bf16)
    pieces = exchanged(mixture.reshape(moe_count, tok, class_width), MOE_CLASS)
    layer_out = (attended.astype(f32) + jnp.sum(pieces.astype(f32), axis=0)).astype(bf16)
    return (attended, layer_out, keys_cache, values_cache)


def solution(mesh):
    far = mesh.shape["seq"] // (PAIR * CORES)
    split = Mesh(
        mesh.devices.reshape(mesh.shape["groups"], far, PAIR, CORES, mesh.shape["rep"]),
        ("groups", "far", "near", "core", "rep"),
    )
    return jax.shard_map(
        body,
        mesh=split,
        in_specs=(
            P(TOKENS, "rep"),
            P(TOKENS, "rep"),
            P(TOKENS, "rep"),
            P(TOKENS, "rep"),
            P(TOKENS, "rep"),
            P("groups"),
            P(TOKENS, "rep"),
            P(SEQ, "rep"),
            P(),
            P(),
            P("rep", None, SEQ),
            P("rep", None, SEQ),
            P("rep", SEQ, None),
            P(TOKENS, None),
        ),
        out_specs=(
            P(TOKENS, "rep"),
            P(TOKENS, "rep"),
            P(TOKENS, None),
            P(TOKENS, None),
        ),
        check_vma=False,
    )
```

```python
import math

import jax
import jax.numpy as jnp
from jax import lax
from jax.sharding import Mesh
from jax.sharding import PartitionSpec as P


EXPERTS = 4
CAP = 12
LANES = 128
PAIR = 2
CORES = 2
SEQ = ("far", "near", "core")
TOKENS = ("groups", "far", "near", "core")
SHARE = ("near", "core")
CLASS = ("far",)
EARLY_PART = 9 / 16


def swapped(array, axis):
    return lax.ppermute(array, axis, [(0, 1), (1, 0)])


def after(array, ready):
    return lax.optimization_barrier((array, ready))[0]


def owners_by(axes):
    place = {a: lax.axis_index(a) for a in SEQ}
    held = [place]
    for axis in axes:
        held = held + [{**p, axis: 1 - p[axis]} for p in held]
    sizes = {a: lax.axis_size(a) for a in SEQ}
    return [(p["far"] * sizes["near"] + p["near"]) * sizes["core"] + p["core"] for p in held]


def exchanged(tiles, axis):
    return lax.all_to_all(tiles, axis, 0, 0, tiled=True)


def sent_to_all(array, axis):
    return exchanged(jnp.broadcast_to(array[None], (lax.axis_size(axis), *array.shape)), axis)


def side_by_side(tiles):
    return jnp.concatenate([tiles[i] for i in range(tiles.shape[0])], axis=1)


def block_lookup(owners, block_order):
    width = block_order.shape[0]
    hits = owners[:, None] == jnp.arange(width, dtype=jnp.int32)[None, :]
    return jnp.sum(jnp.where(hits, block_order[None, :], 0), axis=1)


def class_places(axes):
    sizes = {a: lax.axis_size(a) for a in SEQ}
    count = lax.axis_size(axes)
    index = jnp.arange(count, dtype=jnp.int32)
    place = {a: jnp.full((count,), lax.axis_index(a), jnp.int32) for a in SEQ}
    for axis in reversed(axes):
        place[axis] = index % sizes[axis]
        index = index // sizes[axis]
    return (place["far"] * sizes["near"] + place["near"]) * sizes["core"] + place["core"]


def body(
    queries,
    keys_new,
    values_new,
    keys_past,
    values_past,
    block_order,
    residual,
    out_proj,
    norm_gain,
    router,
    w_gate,
    w_up,
    w_down,
    expert_ids,
):
    bf16, f32 = jnp.bfloat16, jnp.float32
    tok = queries.shape[0]
    head_dim = keys_new.shape[1]
    q_per = queries.shape[1] // head_dim
    width = queries.shape[1]
    past_len = keys_past.shape[0]
    rep_count = lax.axis_size("rep")
    scaling = 1.0 / math.sqrt(head_dim)

    count = lax.axis_size(CLASS)
    rows = count * tok
    kv_local = jnp.concatenate(
        [
            jnp.concatenate([keys_past, keys_new], axis=0),
            jnp.concatenate([values_past, values_new], axis=0),
        ],
        axis=1,
    )
    kv_pair = jnp.concatenate([kv_local, swapped(kv_local, "near")], axis=0)
    kv_all = jnp.concatenate([kv_pair, swapped(kv_pair, "core")], axis=0)
    out_proj_own = lax.all_gather(out_proj, ("far", "near"), axis=0, tiled=True)
    out_proj_other = swapped(out_proj_own, "core")

    ids_wide = jnp.pad(expert_ids.astype(bf16), ((0, 0), (0, LANES - expert_ids.shape[1])))
    query_class = sent_to_all(jnp.concatenate([queries, ids_wide], axis=1), CLASS)
    query_class = query_class.reshape(rows, width + LANES)
    ids = query_class[:, width : width + 2].astype(jnp.int32)
    query_pos = (
        block_lookup(class_places(CLASS), block_order)[:, None] * tok
        + jnp.arange(tok, dtype=jnp.int32)[None, :]
    ).reshape(rows)

    key_span = past_len + tok
    key_owner_pos = block_lookup(jnp.stack(owners_by(SHARE)), block_order)
    offset = jnp.arange(key_span, dtype=jnp.int32) - past_len
    key_pos = jnp.where(
        offset[None, :] >= 0, key_owner_pos[:, None] * tok + offset[None, :], -1
    ).reshape(-1)
    visible = key_pos[None, :] <= query_pos[:, None]
    keys, values = kv_all[:, :head_dim], kv_all[:, head_dim:]
    heads = jnp.stack(
        [query_class[:, j * head_dim : (j + 1) * head_dim] for j in range(q_per)], axis=0
    )
    scores = jnp.einsum("jtd,kd->jtk", heads, keys, preferred_element_type=f32) * scaling
    scores = jnp.where(visible[None], scores, -1e30)
    shift = jnp.max(scores, axis=2).astype(bf16)
    weights = jnp.exp(scores - shift.astype(f32)[:, :, None])
    totals = jnp.sum(weights, axis=2)
    partial = jnp.einsum("jtk,kd->jtd", weights.astype(bf16), values, preferred_element_type=f32)
    totals_high = totals.astype(bf16)
    totals_low = (totals - totals_high.astype(f32)).astype(bf16)
    notes = jnp.concatenate([shift, totals_high, totals_low], axis=0).T
    notes = jnp.pad(notes, ((0, 0), (0, LANES - notes.shape[1])))
    message = jnp.concatenate([partial[j].astype(bf16) for j in range(q_per)] + [notes], axis=1)
    parts = exchanged(message.reshape(count, tok, width + LANES), CLASS)

    model = w_gate.shape[1]
    cut = int(model * EARLY_PART)
    gate_up = jnp.concatenate([w_gate[0], w_up[0]], axis=1)
    down = w_down[0]
    gate_up_core = swapped(gate_up, "core")
    down_core = swapped(down, "core")
    first_pair = swapped(after(gate_up[:cut], parts), "near")
    first_cross = swapped(first_pair, "core")

    part_shift = parts[:, :, width : width + q_per].astype(f32)
    part_total = parts[:, :, width + q_per : width + 2 * q_per].astype(f32) + parts[
        :, :, width + 2 * q_per : width + 3 * q_per
    ].astype(f32)
    level = jnp.exp(part_shift - jnp.max(part_shift, axis=0, keepdims=True))
    total = jnp.sum(level * part_total, axis=0)
    attn_local = jnp.concatenate(
        [
            jnp.sum(
                level[:, :, j : j + 1]
                * parts[:, :, j * head_dim : (j + 1) * head_dim].astype(f32),
                axis=0,
            )
            / total[:, j : j + 1]
            for j in range(q_per)
        ],
        axis=1,
    ).astype(bf16)

    spread = sent_to_all(jnp.concatenate([attn_local, keys_new, values_new], axis=1), "rep")
    keys_cache = side_by_side(spread[:, :, width : width + head_dim])
    values_cache = side_by_side(spread[:, :, width + head_dim :])
    core = lax.axis_index("core")
    rows_of = out_proj.shape[0]
    even, odd = (
        side_by_side(
            jnp.concatenate(
                [spread[:, :, j : j + rows_of] for j in range(first, width, CORES * rows_of)], axis=2
            )
        )
        for first in (0, rows_of)
    )
    projected = jnp.dot(
        jnp.where(core == 0, even, odd), out_proj_own, preferred_element_type=f32
    ) + jnp.dot(jnp.where(core == 0, odd, even), out_proj_other, preferred_element_type=f32)
    attended = (residual.astype(f32) + projected).astype(bf16)

    class_rows = rows
    class_width = attended.shape[1]
    class_attended = sent_to_all(attended, CLASS).reshape(class_rows, class_width)
    second_pair = swapped(after(gate_up[cut:], class_attended), "near")
    down_pair = swapped(after(down, class_attended), "near")
    experts = jnp.arange(EXPERTS, dtype=jnp.int32)
    first_pick = (ids[:, 0:1] == experts[None, :]).astype(f32)
    second_pick = (ids[:, 1:2] == experts[None, :]).astype(f32)
    member = first_pick + second_pick
    row = jnp.arange(class_rows, dtype=jnp.int32)
    earlier = (row[:, None] // tok == row[None, :] // tok) & (row[None, :] < row[:, None])
    ranking = jnp.dot(
        earlier.astype(bf16), member.astype(bf16), preferred_element_type=f32
    ).astype(jnp.int32)
    slot_of = jnp.where(member > 0, (row[:, None] // tok) * CAP + ranking, -1)
    slot_count = count * CAP
    slots = jnp.arange(slot_count, dtype=jnp.int32)
    selection = (slot_of.T[:, None, :] == slots[None, :, None]).astype(bf16)
    slot_rows = jnp.dot(
        selection.reshape(EXPERTS * slot_count, class_rows),
        class_attended,
        preferred_element_type=f32,
    ).astype(bf16)
    slot_rows = slot_rows.reshape(EXPERTS, slot_count, class_width)
    halves = rep_count // EXPERTS
    arrived = exchanged(jnp.concatenate([slot_rows] * halves, axis=0), "rep")
    features = side_by_side(arrived).astype(f32)

    mean_square = jnp.mean(features * features, axis=1, keepdims=True)
    normed = (features * norm_gain[None, :] * lax.rsqrt(mean_square + 1e-05)).astype(bf16)
    logits = jnp.dot(normed.astype(f32), router, precision=lax.Precision.HIGHEST)
    mine = lax.axis_index("rep") % EXPERTS
    my_selection = lax.dynamic_index_in_dim(selection, mine, axis=0, keepdims=False)
    slot_member = jnp.dot(my_selection, member.astype(bf16), preferred_element_type=f32)
    own = (experts == mine)[None, :]
    own_logit = jnp.sum(jnp.where(own, logits, 0.0), axis=1)
    other_logit = jnp.sum(jnp.where(own, 0.0, slot_member * logits), axis=1)
    share = jax.nn.sigmoid(own_logit - other_logit)
    hidden_width = w_gate.shape[2]

    def hidden_of(*parts_of):
        both, at = None, 0
        for part in parts_of:
            piece = jnp.dot(
                normed[:, at : at + part.shape[0]], part, preferred_element_type=f32
            )
            both, at = piece if both is None else both + piece, at + part.shape[0]
        return (jax.nn.silu(both[:, :hidden_width]) * both[:, hidden_width:]).astype(bf16)

    def out_of(hidden, rows_down):
        return jnp.dot(hidden, rows_down, preferred_element_type=f32)

    expert_out = out_of(hidden_of(gate_up), down) + out_of(hidden_of(gate_up_core), down_core)
    second_cross = swapped(after(second_pair, expert_out), "core")
    hidden_pair = hidden_of(first_pair, second_pair)
    down_cross = swapped(after(down_pair, hidden_pair), "core")
    expert_out = expert_out + out_of(hidden_pair, down_pair)
    expert_out = expert_out + out_of(hidden_of(first_cross, second_cross), down_cross)
    weighted = (expert_out * share[:, None]).astype(bf16)
    outgoing = jnp.stack(
        [weighted[:, i * class_width : (i + 1) * class_width] for i in range(rep_count)], axis=0
    )
    returned = exchanged(outgoing, "rep")

    back = jnp.concatenate([selection.reshape(EXPERTS * slot_count, class_rows)] * halves, axis=0)
    mixture = lax.dot_general(
        back,
        returned.reshape(rep_count * slot_count, class_width),
        (((0,), (0,)), ((), ())),
        preferred_element_type=f32,
    ).astype(bf16)
    pieces = exchanged(mixture.reshape(count, tok, class_width), CLASS)
    layer_out = (attended.astype(f32) + jnp.sum(pieces.astype(f32), axis=0)).astype(bf16)
    return (attended, layer_out, keys_cache, values_cache)


def solution(mesh):
    far = mesh.shape["seq"] // (PAIR * CORES)
    split = Mesh(
        mesh.devices.reshape(mesh.shape["groups"], far, PAIR, CORES, mesh.shape["rep"]),
        ("groups", "far", "near", "core", "rep"),
    )
    return jax.shard_map(
        body,
        mesh=split,
        in_specs=(
            P(TOKENS, "rep"),
            P(TOKENS, "rep"),
            P(TOKENS, "rep"),
            P(TOKENS, "rep"),
            P(TOKENS, "rep"),
            P("groups"),
            P(TOKENS, "rep"),
            P(SEQ, "rep"),
            P(),
            P(),
            P("rep", None, SEQ),
            P("rep", None, SEQ),
            P("rep", SEQ, None),
            P(TOKENS, None),
        ),
        out_specs=(
            P(TOKENS, "rep"),
            P(TOKENS, "rep"),
            P(TOKENS, None),
            P(TOKENS, None),
        ),
        check_vma=False,
    )
```

```python
import functools
import math

import jax
import jax.numpy as jnp
from jax import lax
from jax.experimental import pallas as pl
from jax.experimental.pallas import tpu as pltpu
from jax.sharding import Mesh
from jax.sharding import PartitionSpec as P


EXPERTS = 4
CAP = 12
LANES = 128
PAIR = 2
CORES = 2
SEQ = ("far", "near", "core")
TOKENS = ("groups", "far", "near", "core")
SHARE = ("near", "core")
CLASS = ("far",)
EARLY_PART = 9 / 16


def swapped(array, axis):
    return lax.ppermute(array, axis, [(0, 1), (1, 0)])


def after(array, ready):
    return lax.optimization_barrier((array, ready))[0]


def owners_by(axes):
    place = {a: lax.axis_index(a) for a in SEQ}
    held = [place]
    for axis in axes:
        held = held + [{**p, axis: 1 - p[axis]} for p in held]
    sizes = {a: lax.axis_size(a) for a in SEQ}
    return [(p["far"] * sizes["near"] + p["near"]) * sizes["core"] + p["core"] for p in held]


def exchanged(tiles, axis):
    return lax.all_to_all(tiles, axis, 0, 0, tiled=True)


def sent_to_all(array, axis):
    return exchanged(jnp.broadcast_to(array[None], (lax.axis_size(axis), *array.shape)), axis)


def side_by_side(tiles):
    return jnp.concatenate([tiles[i] for i in range(tiles.shape[0])], axis=1)


def block_lookup(owners, block_order):
    width = block_order.shape[0]
    hits = owners[:, None] == jnp.arange(width, dtype=jnp.int32)[None, :]
    return jnp.sum(jnp.where(hits, block_order[None, :], 0), axis=1)


def class_places(axes):
    sizes = {a: lax.axis_size(a) for a in SEQ}
    count = lax.axis_size(axes)
    index = jnp.arange(count, dtype=jnp.int32)
    place = {a: jnp.full((count,), lax.axis_index(a), jnp.int32) for a in SEQ}
    for axis in reversed(axes):
        place[axis] = index % sizes[axis]
        index = index // sizes[axis]
    return (place["far"] * sizes["near"] + place["near"]) * sizes["core"] + place["core"]


def expert_kernel(cuts, final, *refs):
    parts = sum(len(c) for c in cuts)
    x_ref, refs = refs[0], refs[1:]
    if final:
        before_ref, share_ref, refs = refs[0], refs[1], refs[2:]
    gu_refs, refs = refs[:parts], refs[parts:]
    down_refs, refs = refs[: len(cuts)], refs[len(cuts) :]
    out_ref, gu_held, down_held, gu_sem, down_sem = refs
    width = down_refs[0].shape[0]
    copies, k = [], 0
    for d, cut in enumerate(cuts):
        at = 0
        for size in cut:
            copy = pltpu.make_async_copy(
                gu_refs[k], gu_held.at[d, pl.ds(at, size)], gu_sem.at[k]
            )
            copy.start()
            copies.append(copy)
            at, k = at + size, k + 1
    down_copies = []
    for d in range(len(cuts)):
        copy = pltpu.make_async_copy(
            down_refs[d], down_held.at[pl.ds(d * width, width)], down_sem.at[d]
        )
        copy.start()
        down_copies.append(copy)
    hidden, k = [], 0
    for d, cut in enumerate(cuts):
        both, at = None, 0
        for size in cut:
            copies[k].wait()
            piece = jnp.dot(
                x_ref[:, at : at + size],
                gu_held[d, at : at + size, :],
                preferred_element_type=jnp.float32,
            )
            both = piece if both is None else both + piece
            at, k = at + size, k + 1
        gate, up = both[:, :width], both[:, width:]
        hidden.append((gate * jax.nn.sigmoid(gate) * up).astype(jnp.bfloat16))
    hidden = jnp.concatenate(hidden, axis=1)
    for copy in down_copies:
        copy.wait()
    if final:
        tiles, _, columns = out_ref.shape
        for i in range(tiles):
            span = slice(i * columns, (i + 1) * columns)
            piece = jnp.dot(hidden, down_held[:, span], preferred_element_type=jnp.float32)
            out_ref[i] = ((before_ref[:, span] + piece) * share_ref[...]).astype(out_ref.dtype)
    else:
        out_ref[...] = jnp.dot(hidden, down_held[...], preferred_element_type=jnp.float32)


def expert_call(x, gate_ups, downs, out_shape, before=None, share=None):
    cuts = tuple(tuple(g.shape[0] for g in parts) for parts in gate_ups)
    flat = [g for parts in gate_ups for g in parts]
    final = before is not None
    extra = [before, share] if final else []
    vmem = pl.BlockSpec(memory_space=pltpu.VMEM)
    anywhere = pl.BlockSpec(memory_space=pl.ANY)
    return pl.pallas_call(
        functools.partial(expert_kernel, cuts, final),
        out_shape=out_shape,
        in_specs=[vmem] * (1 + len(extra)) + [anywhere] * (len(flat) + len(downs)),
        out_specs=vmem,
        scratch_shapes=[
            pltpu.VMEM((len(cuts), sum(cuts[0]), flat[0].shape[1]), flat[0].dtype),
            pltpu.VMEM((len(downs) * downs[0].shape[0], downs[0].shape[1]), downs[0].dtype),
            pltpu.SemaphoreType.DMA((len(flat),)),
            pltpu.SemaphoreType.DMA((len(downs),)),
        ],
    )(x, *extra, *flat, *downs)


def body(
    queries,
    keys_new,
    values_new,
    keys_past,
    values_past,
    block_order,
    residual,
    out_proj,
    norm_gain,
    router,
    w_gate,
    w_up,
    w_down,
    expert_ids,
):
    bf16, f32 = jnp.bfloat16, jnp.float32
    tok = queries.shape[0]
    head_dim = keys_new.shape[1]
    q_per = queries.shape[1] // head_dim
    width = queries.shape[1]
    past_len = keys_past.shape[0]
    rep_count = lax.axis_size("rep")
    scaling = 1.0 / math.sqrt(head_dim)

    count = lax.axis_size(CLASS)
    rows = count * tok
    kv_local = jnp.concatenate(
        [
            jnp.concatenate([keys_past, keys_new], axis=0),
            jnp.concatenate([values_past, values_new], axis=0),
        ],
        axis=1,
    )
    kv_pair = jnp.concatenate([kv_local, swapped(kv_local, "near")], axis=0)
    kv_all = jnp.concatenate([kv_pair, swapped(kv_pair, "core")], axis=0)
    out_proj_own = lax.all_gather(out_proj, ("far", "near"), axis=0, tiled=True)
    out_proj_other = swapped(out_proj_own, "core")

    ids_wide = jnp.pad(expert_ids.astype(bf16), ((0, 0), (0, LANES - expert_ids.shape[1])))
    query_class = sent_to_all(jnp.concatenate([queries, ids_wide], axis=1), CLASS)
    query_class = query_class.reshape(rows, width + LANES)
    ids = query_class[:, width : width + 2].astype(jnp.int32)
    query_pos = (
        block_lookup(class_places(CLASS), block_order)[:, None] * tok
        + jnp.arange(tok, dtype=jnp.int32)[None, :]
    ).reshape(rows)

    key_span = past_len + tok
    key_owner_pos = block_lookup(jnp.stack(owners_by(SHARE)), block_order)
    offset = jnp.arange(key_span, dtype=jnp.int32) - past_len
    key_pos = jnp.where(
        offset[None, :] >= 0, key_owner_pos[:, None] * tok + offset[None, :], -1
    ).reshape(-1)
    visible = key_pos[None, :] <= query_pos[:, None]
    keys, values = kv_all[:, :head_dim], kv_all[:, head_dim:]
    heads = jnp.stack(
        [query_class[:, j * head_dim : (j + 1) * head_dim] for j in range(q_per)], axis=0
    )
    scores = jnp.einsum("jtd,kd->jtk", heads, keys, preferred_element_type=f32) * scaling
    scores = jnp.where(visible[None], scores, -1e30)
    shift = jnp.max(scores, axis=2).astype(bf16)
    weights = jnp.exp(scores - shift.astype(f32)[:, :, None])
    totals = jnp.sum(weights, axis=2)
    partial = jnp.einsum("jtk,kd->jtd", weights.astype(bf16), values, preferred_element_type=f32)
    totals_high = totals.astype(bf16)
    totals_low = (totals - totals_high.astype(f32)).astype(bf16)
    notes = jnp.concatenate([shift, totals_high, totals_low], axis=0).T
    notes = jnp.pad(notes, ((0, 0), (0, LANES - notes.shape[1])))
    message = jnp.concatenate([partial[j].astype(bf16) for j in range(q_per)] + [notes], axis=1)
    parts = exchanged(message.reshape(count, tok, width + LANES), CLASS)

    model = w_gate.shape[1]
    cut = int(model * EARLY_PART)
    gate_up = jnp.concatenate([w_gate[0], w_up[0]], axis=1)
    down = w_down[0]
    gate_up_core = swapped(gate_up, "core")
    down_core = swapped(down, "core")
    first_pair = swapped(after(gate_up[:cut], parts), "near")
    first_cross = swapped(first_pair, "core")

    part_shift = parts[:, :, width : width + q_per].astype(f32)
    part_total = parts[:, :, width + q_per : width + 2 * q_per].astype(f32) + parts[
        :, :, width + 2 * q_per : width + 3 * q_per
    ].astype(f32)
    level = jnp.exp(part_shift - jnp.max(part_shift, axis=0, keepdims=True))
    total = jnp.sum(level * part_total, axis=0)
    attn_local = jnp.concatenate(
        [
            jnp.sum(
                level[:, :, j : j + 1]
                * parts[:, :, j * head_dim : (j + 1) * head_dim].astype(f32),
                axis=0,
            )
            / total[:, j : j + 1]
            for j in range(q_per)
        ],
        axis=1,
    ).astype(bf16)

    spread = sent_to_all(jnp.concatenate([attn_local, keys_new, values_new], axis=1), "rep")
    keys_cache = side_by_side(spread[:, :, width : width + head_dim])
    values_cache = side_by_side(spread[:, :, width + head_dim :])
    core = lax.axis_index("core")
    rows_of = out_proj.shape[0]
    even, odd = (
        side_by_side(
            jnp.concatenate(
                [spread[:, :, j : j + rows_of] for j in range(first, width, CORES * rows_of)], axis=2
            )
        )
        for first in (0, rows_of)
    )
    projected = jnp.dot(
        jnp.where(core == 0, even, odd), out_proj_own, preferred_element_type=f32
    ) + jnp.dot(jnp.where(core == 0, odd, even), out_proj_other, preferred_element_type=f32)
    attended = (residual.astype(f32) + projected).astype(bf16)

    class_rows = rows
    class_width = attended.shape[1]
    class_attended = sent_to_all(attended, CLASS).reshape(class_rows, class_width)
    second_pair = swapped(after(gate_up[cut:], class_attended), "near")
    down_pair = swapped(after(down, class_attended), "near")
    experts = jnp.arange(EXPERTS, dtype=jnp.int32)
    first_pick = (ids[:, 0:1] == experts[None, :]).astype(f32)
    second_pick = (ids[:, 1:2] == experts[None, :]).astype(f32)
    member = first_pick + second_pick
    row = jnp.arange(class_rows, dtype=jnp.int32)
    earlier = (row[:, None] // tok == row[None, :] // tok) & (row[None, :] < row[:, None])
    ranking = jnp.dot(
        earlier.astype(bf16), member.astype(bf16), preferred_element_type=f32
    ).astype(jnp.int32)
    slot_of = jnp.where(member > 0, (row[:, None] // tok) * CAP + ranking, -1)
    slot_count = count * CAP
    slots = jnp.arange(slot_count, dtype=jnp.int32)
    selection = (slot_of.T[:, None, :] == slots[None, :, None]).astype(bf16)
    slot_rows = jnp.dot(
        selection.reshape(EXPERTS * slot_count, class_rows),
        class_attended,
        preferred_element_type=f32,
    ).astype(bf16)
    slot_rows = slot_rows.reshape(EXPERTS, slot_count, class_width)
    halves = rep_count // EXPERTS
    arrived = exchanged(jnp.concatenate([slot_rows] * halves, axis=0), "rep")
    features = side_by_side(arrived).astype(f32)

    mean_square = jnp.mean(features * features, axis=1, keepdims=True)
    normed = (features * norm_gain[None, :] * lax.rsqrt(mean_square + 1e-05)).astype(bf16)
    logits = jnp.dot(normed.astype(f32), router, precision=lax.Precision.HIGHEST)
    mine = lax.axis_index("rep") % EXPERTS
    my_selection = lax.dynamic_index_in_dim(selection, mine, axis=0, keepdims=False)
    slot_member = jnp.dot(my_selection, member.astype(bf16), preferred_element_type=f32)
    own = (experts == mine)[None, :]
    own_logit = jnp.sum(jnp.where(own, logits, 0.0), axis=1)
    other_logit = jnp.sum(jnp.where(own, 0.0, slot_member * logits), axis=1)
    share = jax.nn.sigmoid(own_logit - other_logit)
    near_out = expert_call(
        normed,
        ((gate_up,), (gate_up_core,)),
        (down, down_core),
        jax.ShapeDtypeStruct((slot_count, model), f32),
    )
    second_cross = swapped(after(second_pair, near_out), "core")
    down_cross = swapped(after(down_pair, near_out), "core")
    outgoing = expert_call(
        normed,
        ((first_pair, second_pair), (first_cross, second_cross)),
        (down_pair, down_cross),
        jax.ShapeDtypeStruct((rep_count, slot_count, class_width), bf16),
        before=near_out,
        share=share[:, None],
    )
    returned = exchanged(outgoing, "rep")

    back = jnp.concatenate([selection.reshape(EXPERTS * slot_count, class_rows)] * halves, axis=0)
    mixture = lax.dot_general(
        back,
        returned.reshape(rep_count * slot_count, class_width),
        (((0,), (0,)), ((), ())),
        preferred_element_type=f32,
    ).astype(bf16)
    pieces = exchanged(mixture.reshape(count, tok, class_width), CLASS)
    layer_out = (attended.astype(f32) + jnp.sum(pieces.astype(f32), axis=0)).astype(bf16)
    return (attended, layer_out, keys_cache, values_cache)


def solution(mesh):
    far = mesh.shape["seq"] // (PAIR * CORES)
    split = Mesh(
        mesh.devices.reshape(mesh.shape["groups"], far, PAIR, CORES, mesh.shape["rep"]),
        ("groups", "far", "near", "core", "rep"),
    )
    return jax.shard_map(
        body,
        mesh=split,
        in_specs=(
            P(TOKENS, "rep"),
            P(TOKENS, "rep"),
            P(TOKENS, "rep"),
            P(TOKENS, "rep"),
            P(TOKENS, "rep"),
            P("groups"),
            P(TOKENS, "rep"),
            P(SEQ, "rep"),
            P(),
            P(),
            P("rep", None, SEQ),
            P("rep", None, SEQ),
            P("rep", SEQ, None),
            P(TOKENS, None),
        ),
        out_specs=(
            P(TOKENS, "rep"),
            P(TOKENS, "rep"),
            P(TOKENS, None),
            P(TOKENS, None),
        ),
        check_vma=False,
    )
```

```python
import functools
import math

import jax
import jax.numpy as jnp
from jax import lax
from jax.experimental import pallas as pl
from jax.experimental.pallas import tpu as pltpu
from jax.sharding import Mesh
from jax.sharding import PartitionSpec as P


EXPERTS = 4
CAP = 12
LANES = 128
PAIR = 2
CORES = 2
SEQ = ("far", "near", "core")
TOKENS = ("groups", "far", "near", "core")
SHARE = ("near", "core")
CLASS = ("far",)
EARLY_PART = 9 / 16


def swapped(array, axis):
    return lax.ppermute(array, axis, [(0, 1), (1, 0)])


def after(array, ready):
    return lax.optimization_barrier((array, ready))[0]


def owners_by(axes):
    place = {a: lax.axis_index(a) for a in SEQ}
    held = [place]
    for axis in axes:
        held = held + [{**p, axis: 1 - p[axis]} for p in held]
    sizes = {a: lax.axis_size(a) for a in SEQ}
    return [(p["far"] * sizes["near"] + p["near"]) * sizes["core"] + p["core"] for p in held]


def exchanged(tiles, axis):
    return lax.all_to_all(tiles, axis, 0, 0, tiled=True)


def sent_to_all(array, axis):
    return exchanged(jnp.broadcast_to(array[None], (lax.axis_size(axis), *array.shape)), axis)


def side_by_side(tiles):
    return jnp.concatenate([tiles[i] for i in range(tiles.shape[0])], axis=1)


def block_lookup(owners, block_order):
    width = block_order.shape[0]
    hits = owners[:, None] == jnp.arange(width, dtype=jnp.int32)[None, :]
    return jnp.sum(jnp.where(hits, block_order[None, :], 0), axis=1)


def class_places(axes):
    sizes = {a: lax.axis_size(a) for a in SEQ}
    count = lax.axis_size(axes)
    index = jnp.arange(count, dtype=jnp.int32)
    place = {a: jnp.full((count,), lax.axis_index(a), jnp.int32) for a in SEQ}
    for axis in reversed(axes):
        place[axis] = index % sizes[axis]
        index = index // sizes[axis]
    return (place["far"] * sizes["near"] + place["near"]) * sizes["core"] + place["core"]


def _chunks(size, most=1024):
    count = -(-size // most)
    while size % (count * LANES) and count < size // LANES:
        count += 1
    return [(i * (size // count), size // count) for i in range(count)]


def expert_kernel(cuts, final, *refs):
    parts = sum(len(c) for c in cuts)
    chunks = [[_chunks(size) for size in cut] for cut in cuts]
    x_ref, refs = refs[0], refs[1:]
    if final:
        before_ref, share_ref, refs = refs[0], refs[1], refs[2:]
    gu_refs, refs = refs[:parts], refs[parts:]
    down_refs, refs = refs[: len(cuts)], refs[len(cuts) :]
    out_ref, gu_held, down_held, gu_sem, down_sem = refs
    width = down_refs[0].shape[0]
    copies, k = [], 0
    for d, cut in enumerate(cuts):
        at = 0
        for p, size in enumerate(cut):
            for first, length in chunks[d][p]:
                copy = pltpu.make_async_copy(
                    gu_refs[k].at[pl.ds(first, length)],
                    gu_held.at[d, pl.ds(at + first, length)],
                    gu_sem.at[len(copies)],
                )
                copy.start()
                copies.append(copy)
            at, k = at + size, k + 1
    down_copies = []
    for d in range(len(cuts)):
        copy = pltpu.make_async_copy(
            down_refs[d], down_held.at[pl.ds(d * width, width)], down_sem.at[d]
        )
        copy.start()
        down_copies.append(copy)
    hidden, k = [], 0
    for d, cut in enumerate(cuts):
        both, at = None, 0
        for p, size in enumerate(cut):
            for first, length in chunks[d][p]:
                copies[k].wait()
                span = slice(at + first, at + first + length)
                piece = jnp.dot(
                    x_ref[:, span], gu_held[d, span, :], preferred_element_type=jnp.float32
                )
                both = piece if both is None else both + piece
                k += 1
            at += size
        gate, up = both[:, :width], both[:, width:]
        hidden.append((gate * jax.nn.sigmoid(gate) * up).astype(jnp.bfloat16))
    hidden = jnp.concatenate(hidden, axis=1)
    for copy in down_copies:
        copy.wait()
    if final:
        tiles, _, columns = out_ref.shape
        for i in range(tiles):
            span = slice(i * columns, (i + 1) * columns)
            piece = jnp.dot(hidden, down_held[:, span], preferred_element_type=jnp.float32)
            out_ref[i] = ((before_ref[:, span] + piece) * share_ref[...]).astype(out_ref.dtype)
    else:
        out_ref[...] = jnp.dot(hidden, down_held[...], preferred_element_type=jnp.float32)


def expert_call(x, gate_ups, downs, out_shape, before=None, share=None):
    cuts = tuple(tuple(g.shape[0] for g in parts) for parts in gate_ups)
    flat = [g for parts in gate_ups for g in parts]
    final = before is not None
    extra = [before, share] if final else []
    vmem = pl.BlockSpec(memory_space=pltpu.VMEM)
    anywhere = pl.BlockSpec(memory_space=pl.ANY)
    return pl.pallas_call(
        functools.partial(expert_kernel, cuts, final),
        out_shape=out_shape,
        in_specs=[vmem] * (1 + len(extra)) + [anywhere] * (len(flat) + len(downs)),
        out_specs=vmem,
        scratch_shapes=[
            pltpu.VMEM((len(cuts), sum(cuts[0]), flat[0].shape[1]), flat[0].dtype),
            pltpu.VMEM((len(downs) * downs[0].shape[0], downs[0].shape[1]), downs[0].dtype),
            pltpu.SemaphoreType.DMA((sum(len(_chunks(g.shape[0])) for g in flat),)),
            pltpu.SemaphoreType.DMA((len(downs),)),
        ],
    )(x, *extra, *flat, *downs)


def body(
    queries,
    keys_new,
    values_new,
    keys_past,
    values_past,
    block_order,
    residual,
    out_proj,
    norm_gain,
    router,
    w_gate,
    w_up,
    w_down,
    expert_ids,
):
    bf16, f32 = jnp.bfloat16, jnp.float32
    tok = queries.shape[0]
    head_dim = keys_new.shape[1]
    q_per = queries.shape[1] // head_dim
    width = queries.shape[1]
    past_len = keys_past.shape[0]
    rep_count = lax.axis_size("rep")
    scaling = 1.0 / math.sqrt(head_dim)

    count = lax.axis_size(CLASS)
    rows = count * tok
    kv_local = jnp.concatenate(
        [
            jnp.concatenate([keys_past, keys_new], axis=0),
            jnp.concatenate([values_past, values_new], axis=0),
        ],
        axis=1,
    )
    kv_pair = jnp.concatenate([kv_local, swapped(kv_local, "near")], axis=0)
    kv_all = jnp.concatenate([kv_pair, swapped(kv_pair, "core")], axis=0)
    out_proj_own = lax.all_gather(out_proj, ("far", "near"), axis=0, tiled=True)
    out_proj_other = swapped(out_proj_own, "core")

    ids_wide = jnp.pad(expert_ids.astype(bf16), ((0, 0), (0, LANES - expert_ids.shape[1])))
    query_class = sent_to_all(jnp.concatenate([queries, ids_wide], axis=1), CLASS)
    query_class = query_class.reshape(rows, width + LANES)
    ids = query_class[:, width : width + 2].astype(jnp.int32)
    query_pos = (
        block_lookup(class_places(CLASS), block_order)[:, None] * tok
        + jnp.arange(tok, dtype=jnp.int32)[None, :]
    ).reshape(rows)

    key_span = past_len + tok
    key_owner_pos = block_lookup(jnp.stack(owners_by(SHARE)), block_order)
    offset = jnp.arange(key_span, dtype=jnp.int32) - past_len
    key_pos = jnp.where(
        offset[None, :] >= 0, key_owner_pos[:, None] * tok + offset[None, :], -1
    ).reshape(-1)
    visible = key_pos[None, :] <= query_pos[:, None]
    keys, values = kv_all[:, :head_dim], kv_all[:, head_dim:]
    heads = jnp.stack(
        [query_class[:, j * head_dim : (j + 1) * head_dim] for j in range(q_per)], axis=0
    )
    scores = jnp.einsum("jtd,kd->jtk", heads, keys, preferred_element_type=f32) * scaling
    scores = jnp.where(visible[None], scores, -1e30)
    shift = jnp.max(scores, axis=2).astype(bf16)
    weights = jnp.exp(scores - shift.astype(f32)[:, :, None])
    totals = jnp.sum(weights, axis=2)
    partial = jnp.einsum("jtk,kd->jtd", weights.astype(bf16), values, preferred_element_type=f32)
    totals_high = totals.astype(bf16)
    totals_low = (totals - totals_high.astype(f32)).astype(bf16)
    notes = jnp.concatenate([shift, totals_high, totals_low], axis=0).T
    notes = jnp.pad(notes, ((0, 0), (0, LANES - notes.shape[1])))
    message = jnp.concatenate([partial[j].astype(bf16) for j in range(q_per)] + [notes], axis=1)
    parts = exchanged(message.reshape(count, tok, width + LANES), CLASS)

    model = w_gate.shape[1]
    cut = int(model * EARLY_PART)
    gate_up = jnp.concatenate([w_gate[0], w_up[0]], axis=1)
    down = w_down[0]
    gate_up_core = swapped(gate_up, "core")
    down_core = swapped(down, "core")
    first_pair = swapped(after(gate_up[:cut], parts), "near")
    first_cross = swapped(first_pair, "core")

    part_shift = parts[:, :, width : width + q_per].astype(f32)
    part_total = parts[:, :, width + q_per : width + 2 * q_per].astype(f32) + parts[
        :, :, width + 2 * q_per : width + 3 * q_per
    ].astype(f32)
    level = jnp.exp(part_shift - jnp.max(part_shift, axis=0, keepdims=True))
    total = jnp.sum(level * part_total, axis=0)
    attn_local = jnp.concatenate(
        [
            jnp.sum(
                level[:, :, j : j + 1]
                * parts[:, :, j * head_dim : (j + 1) * head_dim].astype(f32),
                axis=0,
            )
            / total[:, j : j + 1]
            for j in range(q_per)
        ],
        axis=1,
    ).astype(bf16)

    spread = sent_to_all(jnp.concatenate([attn_local, keys_new, values_new], axis=1), "rep")
    keys_cache = side_by_side(spread[:, :, width : width + head_dim])
    values_cache = side_by_side(spread[:, :, width + head_dim :])
    core = lax.axis_index("core")
    rows_of = out_proj.shape[0]
    even, odd = (
        side_by_side(
            jnp.concatenate(
                [spread[:, :, j : j + rows_of] for j in range(first, width, CORES * rows_of)], axis=2
            )
        )
        for first in (0, rows_of)
    )
    projected = jnp.dot(
        jnp.where(core == 0, even, odd), out_proj_own, preferred_element_type=f32
    ) + jnp.dot(jnp.where(core == 0, odd, even), out_proj_other, preferred_element_type=f32)
    attended = (residual.astype(f32) + projected).astype(bf16)
    down_both = lax.all_gather(after(down, out_proj_own), "near", axis=0, tiled=True)
    down_pair = lax.dynamic_slice_in_dim(
        down_both, (1 - lax.axis_index("near")) * down.shape[0], down.shape[0]
    )
    down_cross = swapped(down_pair, "core")

    class_rows = rows
    class_width = attended.shape[1]
    class_attended = sent_to_all(attended, CLASS).reshape(class_rows, class_width)
    second_pair = swapped(after(gate_up[cut:], class_attended), "near")
    experts = jnp.arange(EXPERTS, dtype=jnp.int32)
    first_pick = (ids[:, 0:1] == experts[None, :]).astype(f32)
    second_pick = (ids[:, 1:2] == experts[None, :]).astype(f32)
    member = first_pick + second_pick
    row = jnp.arange(class_rows, dtype=jnp.int32)
    earlier = (row[:, None] // tok == row[None, :] // tok) & (row[None, :] < row[:, None])
    ranking = jnp.dot(
        earlier.astype(bf16), member.astype(bf16), preferred_element_type=f32
    ).astype(jnp.int32)
    slot_of = jnp.where(member > 0, (row[:, None] // tok) * CAP + ranking, -1)
    slot_count = count * CAP
    slots = jnp.arange(slot_count, dtype=jnp.int32)
    selection = (slot_of.T[:, None, :] == slots[None, :, None]).astype(bf16)
    slot_rows = jnp.dot(
        selection.reshape(EXPERTS * slot_count, class_rows),
        class_attended,
        preferred_element_type=f32,
    ).astype(bf16)
    slot_rows = slot_rows.reshape(EXPERTS, slot_count, class_width)
    halves = rep_count // EXPERTS
    arrived = exchanged(jnp.concatenate([slot_rows] * halves, axis=0), "rep")
    features = side_by_side(arrived).astype(f32)

    mean_square = jnp.mean(features * features, axis=1, keepdims=True)
    normed = (features * norm_gain[None, :] * lax.rsqrt(mean_square + 1e-05)).astype(bf16)
    logits = jnp.dot(normed.astype(f32), router, precision=lax.Precision.HIGHEST)
    mine = lax.axis_index("rep") % EXPERTS
    my_selection = lax.dynamic_index_in_dim(selection, mine, axis=0, keepdims=False)
    slot_member = jnp.dot(my_selection, member.astype(bf16), preferred_element_type=f32)
    own = (experts == mine)[None, :]
    own_logit = jnp.sum(jnp.where(own, logits, 0.0), axis=1)
    other_logit = jnp.sum(jnp.where(own, 0.0, slot_member * logits), axis=1)
    share = jax.nn.sigmoid(own_logit - other_logit)
    near_out = expert_call(
        normed,
        ((gate_up,), (gate_up_core,)),
        (down, down_core),
        jax.ShapeDtypeStruct((slot_count, model), f32),
    )
    second_cross = swapped(after(second_pair, near_out), "core")
    outgoing = expert_call(
        normed,
        ((first_pair, second_pair), (first_cross, second_cross)),
        (down_pair, down_cross),
        jax.ShapeDtypeStruct((rep_count, slot_count, class_width), bf16),
        before=near_out,
        share=share[:, None],
    )
    returned = exchanged(outgoing, "rep")

    back = jnp.concatenate([selection.reshape(EXPERTS * slot_count, class_rows)] * halves, axis=0)
    mixture = lax.dot_general(
        back,
        returned.reshape(rep_count * slot_count, class_width),
        (((0,), (0,)), ((), ())),
        preferred_element_type=f32,
    ).astype(bf16)
    pieces = exchanged(mixture.reshape(count, tok, class_width), CLASS)
    layer_out = (attended.astype(f32) + jnp.sum(pieces.astype(f32), axis=0)).astype(bf16)
    return (attended, layer_out, keys_cache, values_cache)


def solution(mesh):
    far = mesh.shape["seq"] // (PAIR * CORES)
    split = Mesh(
        mesh.devices.reshape(mesh.shape["groups"], far, PAIR, CORES, mesh.shape["rep"]),
        ("groups", "far", "near", "core", "rep"),
    )
    return jax.shard_map(
        body,
        mesh=split,
        in_specs=(
            P(TOKENS, "rep"),
            P(TOKENS, "rep"),
            P(TOKENS, "rep"),
            P(TOKENS, "rep"),
            P(TOKENS, "rep"),
            P("groups"),
            P(TOKENS, "rep"),
            P(SEQ, "rep"),
            P(),
            P(),
            P("rep", None, SEQ),
            P("rep", None, SEQ),
            P("rep", SEQ, None),
            P(TOKENS, None),
        ),
        out_specs=(
            P(TOKENS, "rep"),
            P(TOKENS, "rep"),
            P(TOKENS, None),
            P(TOKENS, None),
        ),
        check_vma=False,
    )
```

```python
import functools
import math

import jax
import jax.numpy as jnp
from jax import lax
from jax.experimental import pallas as pl
from jax.experimental.pallas import tpu as pltpu
from jax.sharding import Mesh
from jax.sharding import PartitionSpec as P


EXPERTS = 4
CAP = 12
LANES = 128
PAIR = 2
CORES = 2
SEQ = ("far", "near", "core")
TOKENS = ("groups", "far", "near", "core")
SHARE = ("near", "core")
CLASS = ("far",)
EARLY_PART = 9 / 16


def swapped(array, axis):
    return lax.ppermute(array, axis, [(0, 1), (1, 0)])


def after(array, ready):
    return lax.optimization_barrier((array, ready))[0]


def owners_by(axes):
    place = {a: lax.axis_index(a) for a in SEQ}
    held = [place]
    for axis in axes:
        held = held + [{**p, axis: 1 - p[axis]} for p in held]
    sizes = {a: lax.axis_size(a) for a in SEQ}
    return [(p["far"] * sizes["near"] + p["near"]) * sizes["core"] + p["core"] for p in held]


def exchanged(tiles, axis):
    return lax.all_to_all(tiles, axis, 0, 0, tiled=True)


def sent_to_all(array, axis):
    return exchanged(jnp.broadcast_to(array[None], (lax.axis_size(axis), *array.shape)), axis)


def side_by_side(tiles):
    return jnp.concatenate([tiles[i] for i in range(tiles.shape[0])], axis=1)


def block_lookup(owners, block_order):
    width = block_order.shape[0]
    hits = owners[:, None] == jnp.arange(width, dtype=jnp.int32)[None, :]
    return jnp.sum(jnp.where(hits, block_order[None, :], 0), axis=1)


def class_places(axes):
    sizes = {a: lax.axis_size(a) for a in SEQ}
    count = lax.axis_size(axes)
    index = jnp.arange(count, dtype=jnp.int32)
    place = {a: jnp.full((count,), lax.axis_index(a), jnp.int32) for a in SEQ}
    for axis in reversed(axes):
        place[axis] = index % sizes[axis]
        index = index // sizes[axis]
    return (place["far"] * sizes["near"] + place["near"]) * sizes["core"] + place["core"]


def dot(a, b):
    return jnp.dot(a, b, preferred_element_type=jnp.float32)


def hidden_units(x_ref, parts_of_each):
    both, at = None, 0
    for refs in zip(*parts_of_each):
        size = refs[0].shape[0]
        piece = dot(
            x_ref[:, at : at + size], jnp.concatenate([ref[...] for ref in refs], axis=1)
        )
        both, at = piece if both is None else both + piece, at + size
    width = refs[0].shape[1] // 2
    hidden = []
    for i in range(len(refs)):
        gate = both[:, 2 * i * width : (2 * i + 1) * width]
        up = both[:, (2 * i + 1) * width : (2 * i + 2) * width]
        hidden.append((gate * jax.nn.sigmoid(gate) * up).astype(jnp.bfloat16))
    return jnp.concatenate(hidden, axis=1)


def first_expert_kernel(
    tiles_ref, gain_ref, router_ref, sign_ref, gu_refs, down_refs, out_ref, x_ref, share_ref
):
    count, _, columns = tiles_ref.shape
    squares = 0.0
    for i in range(count):
        tile = tiles_ref[i].astype(jnp.float32)
        squares = squares + jnp.sum(tile * tile, axis=1, keepdims=True)
    scale = lax.rsqrt(squares / (count * columns) + 1e-05)
    logit = 0.0
    for i in range(count):
        span = slice(i * columns, (i + 1) * columns)
        tile = tiles_ref[i].astype(jnp.float32) * gain_ref[:, span] * scale
        x_ref[:, span] = tile.astype(jnp.bfloat16)
        rounded = x_ref[:, span].astype(jnp.float32)
        for e in range(EXPERTS):
            part = jnp.sum(rounded * router_ref[e : e + 1, span], axis=1, keepdims=True)
            logit = logit + part * sign_ref[:, e : e + 1]
    share_ref[...] = jax.nn.sigmoid(logit)
    hidden = hidden_units(x_ref, [(ref,) for ref in gu_refs])
    for i in range(count):
        span = slice(i * columns, (i + 1) * columns)
        out_ref[:, span] = dot(
            hidden, jnp.concatenate([ref[:, span] for ref in down_refs], axis=0)
        )


def last_expert_kernel(x_ref, before_ref, share_ref, gu_refs, down_refs, out_ref):
    count, _, columns = out_ref.shape
    hidden = hidden_units(x_ref, gu_refs)
    for i in range(count):
        span = slice(i * columns, (i + 1) * columns)
        piece = before_ref[:, span] + dot(
            hidden, jnp.concatenate([ref[:, span] for ref in down_refs], axis=0)
        )
        out_ref[i] = (piece * share_ref[...]).astype(out_ref.dtype)


def heads_of(spread_ref, i, rows, width, other):
    even = [spread_ref[i, :, j : j + rows] for j in range(0, width, CORES * rows)]
    odd = [spread_ref[i, :, j : j + rows] for j in range(rows, width, CORES * rows)]
    turn = (lax.axis_index("core") + other) % CORES == 0
    return jnp.where(turn, jnp.concatenate(even, axis=1), jnp.concatenate(odd, axis=1))


def project(spread_ref, proj_ref, rows, width, other):
    count = spread_ref.shape[0]
    depth = width // CORES
    total = None
    for i in range(count):
        piece = dot(
            heads_of(spread_ref, i, rows, width, other), proj_ref[i * depth : (i + 1) * depth, :]
        )
        total = piece if total is None else total + piece
    return total


def own_projection_kernel(rows, width, spread_ref, proj_ref, out_ref):
    out_ref[...] = project(spread_ref, proj_ref, rows, width, 0)


def other_projection_kernel(
    rows, width, spread_ref, proj_ref, before_ref, residual_ref, out_ref, copies_ref
):
    total = before_ref[...] + project(spread_ref, proj_ref, rows, width, 1)
    attended = (residual_ref[...].astype(jnp.float32) + total).astype(out_ref.dtype)
    out_ref[...] = attended
    for i in range(copies_ref.shape[0]):
        copies_ref[i] = attended


def in_vmem(kernel, out_shape, *operands):
    whole = pl.BlockSpec(memory_space=pltpu.VMEM)
    return pl.pallas_call(
        kernel,
        out_shape=out_shape,
        in_specs=jax.tree.map(lambda _: whole, operands),
        out_specs=jax.tree.map(lambda _: whole, out_shape),
    )(*operands)


def body(
    queries,
    keys_new,
    values_new,
    keys_past,
    values_past,
    block_order,
    residual,
    out_proj,
    norm_gain,
    router,
    w_gate,
    w_up,
    w_down,
    expert_ids,
):
    bf16, f32 = jnp.bfloat16, jnp.float32
    tok = queries.shape[0]
    head_dim = keys_new.shape[1]
    q_per = queries.shape[1] // head_dim
    width = queries.shape[1]
    past_len = keys_past.shape[0]
    rep_count = lax.axis_size("rep")
    scaling = 1.0 / math.sqrt(head_dim)

    count = lax.axis_size(CLASS)
    rows = count * tok
    kv_local = jnp.concatenate(
        [
            jnp.concatenate([keys_past, keys_new], axis=0),
            jnp.concatenate([values_past, values_new], axis=0),
        ],
        axis=1,
    )
    kv_pair = jnp.concatenate([kv_local, swapped(kv_local, "near")], axis=0)
    kv_all = jnp.concatenate([kv_pair, swapped(kv_pair, "core")], axis=0)
    out_proj_own = lax.all_gather(out_proj, ("far", "near"), axis=0, tiled=True)
    out_proj_other = swapped(out_proj_own, "core")

    ids_wide = jnp.pad(expert_ids.astype(bf16), ((0, 0), (0, LANES - expert_ids.shape[1])))
    query_class = sent_to_all(jnp.concatenate([queries, ids_wide], axis=1), CLASS)
    query_class = query_class.reshape(rows, width + LANES)
    ids = query_class[:, width : width + 2].astype(jnp.int32)
    query_pos = (
        block_lookup(class_places(CLASS), block_order)[:, None] * tok
        + jnp.arange(tok, dtype=jnp.int32)[None, :]
    ).reshape(rows)

    key_span = past_len + tok
    key_owner_pos = block_lookup(jnp.stack(owners_by(SHARE)), block_order)
    offset = jnp.arange(key_span, dtype=jnp.int32) - past_len
    key_pos = jnp.where(
        offset[None, :] >= 0, key_owner_pos[:, None] * tok + offset[None, :], -1
    ).reshape(-1)
    visible = key_pos[None, :] <= query_pos[:, None]
    keys, values = kv_all[:, :head_dim], kv_all[:, head_dim:]
    heads = jnp.stack(
        [query_class[:, j * head_dim : (j + 1) * head_dim] for j in range(q_per)], axis=0
    )
    scores = jnp.einsum("jtd,kd->jtk", heads, keys, preferred_element_type=f32) * scaling
    scores = jnp.where(visible[None], scores, -1e30)
    shift = jnp.max(scores, axis=2).astype(bf16)
    weights = jnp.exp(scores - shift.astype(f32)[:, :, None])
    totals = jnp.sum(weights, axis=2)
    partial = jnp.einsum("jtk,kd->jtd", weights.astype(bf16), values, preferred_element_type=f32)
    totals_high = totals.astype(bf16)
    totals_low = (totals - totals_high.astype(f32)).astype(bf16)
    notes = jnp.concatenate([shift, totals_high, totals_low], axis=0).T
    notes = jnp.pad(notes, ((0, 0), (0, LANES - notes.shape[1])))
    message = jnp.concatenate([partial[j].astype(bf16) for j in range(q_per)] + [notes], axis=1)
    parts = exchanged(message.reshape(count, tok, width + LANES), CLASS)

    model = w_gate.shape[1]
    cut = int(model * EARLY_PART)
    gate_up = jnp.concatenate([w_gate[0], w_up[0]], axis=1)
    down = w_down[0]
    gate_up_core = swapped(gate_up, "core")
    down_core = swapped(down, "core")
    first_pair = swapped(after(gate_up[:cut], parts), "near")
    first_cross = swapped(first_pair, "core")

    part_shift = parts[:, :, width : width + q_per].astype(f32)
    part_total = parts[:, :, width + q_per : width + 2 * q_per].astype(f32) + parts[
        :, :, width + 2 * q_per : width + 3 * q_per
    ].astype(f32)
    level = jnp.exp(part_shift - jnp.max(part_shift, axis=0, keepdims=True))
    total = jnp.sum(level * part_total, axis=0)
    attn_local = jnp.concatenate(
        [
            jnp.sum(
                level[:, :, j : j + 1]
                * parts[:, :, j * head_dim : (j + 1) * head_dim].astype(f32),
                axis=0,
            )
            / total[:, j : j + 1]
            for j in range(q_per)
        ],
        axis=1,
    ).astype(bf16)

    spread = sent_to_all(jnp.concatenate([attn_local, keys_new, values_new], axis=1), "rep")
    keys_cache = side_by_side(spread[:, :, width : width + head_dim])
    values_cache = side_by_side(spread[:, :, width + head_dim :])
    shape = jax.ShapeDtypeStruct
    sizes = (out_proj.shape[0], width)
    own_part = in_vmem(
        functools.partial(own_projection_kernel, *sizes),
        shape(residual.shape, f32),
        spread,
        out_proj_own,
    )
    attended, attended_copies = in_vmem(
        functools.partial(other_projection_kernel, *sizes),
        (shape(residual.shape, bf16), shape((count, *residual.shape), bf16)),
        spread,
        out_proj_other,
        own_part,
        residual,
    )
    down_both = lax.all_gather(after(down, out_proj_own), "near", axis=0, tiled=True)
    down_pair = lax.dynamic_slice_in_dim(
        down_both, (1 - lax.axis_index("near")) * down.shape[0], down.shape[0]
    )
    down_cross = swapped(down_pair, "core")

    class_rows = rows
    class_width = attended.shape[1]
    class_attended = exchanged(attended_copies, CLASS).reshape(class_rows, class_width)
    second_pair = swapped(after(gate_up[cut:], class_attended), "near")
    experts = jnp.arange(EXPERTS, dtype=jnp.int32)
    first_pick = (ids[:, 0:1] == experts[None, :]).astype(f32)
    second_pick = (ids[:, 1:2] == experts[None, :]).astype(f32)
    member = first_pick + second_pick
    row = jnp.arange(class_rows, dtype=jnp.int32)
    earlier = (row[:, None] // tok == row[None, :] // tok) & (row[None, :] < row[:, None])
    ranking = jnp.dot(
        earlier.astype(bf16), member.astype(bf16), preferred_element_type=f32
    ).astype(jnp.int32)
    slot_of = jnp.where(member > 0, (row[:, None] // tok) * CAP + ranking, -1)
    slot_count = count * CAP
    slots = jnp.arange(slot_count, dtype=jnp.int32)
    selection = (slot_of.T[:, None, :] == slots[None, :, None]).astype(bf16)
    halves = rep_count // EXPERTS
    back = jnp.concatenate([selection.reshape(EXPERTS * slot_count, class_rows)] * halves, axis=0)
    slot_rows = dot(back, class_attended).astype(bf16)
    arrived = exchanged(slot_rows.reshape(rep_count, slot_count, class_width), "rep")

    mine = lax.axis_index("rep") % EXPERTS
    my_selection = lax.dynamic_index_in_dim(selection, mine, axis=0, keepdims=False)
    slot_member = jnp.dot(my_selection, member.astype(bf16), preferred_element_type=f32)
    sign = jnp.where((experts == mine)[None, :], slot_member, -slot_member)
    near_out, normed, share = in_vmem(
        first_expert_kernel,
        (
            shape((slot_count, model), f32),
            shape((slot_count, model), bf16),
            shape((slot_count, 1), f32),
        ),
        arrived,
        norm_gain[None, :],
        router.T,
        sign,
        (gate_up, gate_up_core),
        (down, down_core),
    )
    second_cross = swapped(after(second_pair, near_out), "core")
    outgoing = in_vmem(
        last_expert_kernel,
        shape((rep_count, slot_count, class_width), bf16),
        normed,
        near_out,
        share,
        ((first_pair, second_pair), (first_cross, second_cross)),
        (down_pair, down_cross),
    )
    returned = exchanged(outgoing, "rep")

    mixture = lax.dot_general(
        back,
        returned.reshape(rep_count * slot_count, class_width),
        (((0,), (0,)), ((), ())),
        preferred_element_type=f32,
    ).astype(bf16)
    pieces = exchanged(mixture.reshape(count, tok, class_width), CLASS)
    layer_out = (attended.astype(f32) + jnp.sum(pieces.astype(f32), axis=0)).astype(bf16)
    return (attended, layer_out, keys_cache, values_cache)


def solution(mesh):
    far = mesh.shape["seq"] // (PAIR * CORES)
    split = Mesh(
        mesh.devices.reshape(mesh.shape["groups"], far, PAIR, CORES, mesh.shape["rep"]),
        ("groups", "far", "near", "core", "rep"),
    )
    return jax.shard_map(
        body,
        mesh=split,
        in_specs=(
            P(TOKENS, "rep"),
            P(TOKENS, "rep"),
            P(TOKENS, "rep"),
            P(TOKENS, "rep"),
            P(TOKENS, "rep"),
            P("groups"),
            P(TOKENS, "rep"),
            P(SEQ, "rep"),
            P(),
            P(),
            P("rep", None, SEQ),
            P("rep", None, SEQ),
            P("rep", SEQ, None),
            P(TOKENS, None),
        ),
        out_specs=(
            P(TOKENS, "rep"),
            P(TOKENS, "rep"),
            P(TOKENS, None),
            P(TOKENS, None),
        ),
        check_vma=False,
    )
```

```python
import functools
import math

import jax
import jax.numpy as jnp
from jax import lax
from jax.experimental import pallas as pl
from jax.experimental.pallas import tpu as pltpu
from jax.sharding import Mesh
from jax.sharding import PartitionSpec as P


EXPERTS = 4
CAP = 12
LANES = 128
PAIR = 2
CORES = 2
SEQ = ("far", "near", "core")
TOKENS = ("groups", "far", "near", "core")
SHARE = ("near", "core")
CLASS = ("far",)
CUTS = (4 / 16, 13 / 16)


def swapped(array, axis):
    return lax.ppermute(array, axis, [(0, 1), (1, 0)])


def after(array, ready):
    return lax.optimization_barrier((array, ready))[0]


def owners_by(axes):
    place = {a: lax.axis_index(a) for a in SEQ}
    held = [place]
    for axis in axes:
        held = held + [{**p, axis: 1 - p[axis]} for p in held]
    sizes = {a: lax.axis_size(a) for a in SEQ}
    return [(p["far"] * sizes["near"] + p["near"]) * sizes["core"] + p["core"] for p in held]


def exchanged(tiles, axis):
    return lax.all_to_all(tiles, axis, 0, 0, tiled=True)


def sent_to_all(array, axis):
    return exchanged(jnp.broadcast_to(array[None], (lax.axis_size(axis), *array.shape)), axis)


def side_by_side(tiles):
    return jnp.concatenate([tiles[i] for i in range(tiles.shape[0])], axis=1)


def block_lookup(owners, block_order):
    width = block_order.shape[0]
    hits = owners[:, None] == jnp.arange(width, dtype=jnp.int32)[None, :]
    return jnp.sum(jnp.where(hits, block_order[None, :], 0), axis=1)


def class_places(axes):
    sizes = {a: lax.axis_size(a) for a in SEQ}
    count = lax.axis_size(axes)
    index = jnp.arange(count, dtype=jnp.int32)
    place = {a: jnp.full((count,), lax.axis_index(a), jnp.int32) for a in SEQ}
    for axis in reversed(axes):
        place[axis] = index % sizes[axis]
        index = index // sizes[axis]
    return (place["far"] * sizes["near"] + place["near"]) * sizes["core"] + place["core"]


def dot(a, b):
    return jnp.dot(a, b, preferred_element_type=jnp.float32)


def row_chunks(parts_of_each):
    edges = {0}
    for parts in parts_of_each:
        at = 0
        for size in parts:
            edges.add(at + size)
            at += size
    edges = sorted(edges)
    fine = [edges[0]]
    for edge in edges[1:]:
        while edge - fine[-1] > 1280:
            fine.append(fine[-1] + 1024)
        fine.append(edge)
    chunks = []
    for first, last in zip(fine, fine[1:]):
        sources = []
        for parts in parts_of_each:
            at = 0
            for k, size in enumerate(parts):
                if at <= first < at + size:
                    sources.append((k, first - at))
                at += size
        chunks.append((first, last - first, sources))
    return chunks


def expert_kernel(
    tiles_ref,
    gain_ref,
    router_ref,
    sign_ref,
    gu_refs,
    down_refs,
    out_ref,
    x_ref,
    both_ref,
    gu_held,
    down_held,
    gu_sem,
    down_sem,
):
    count, _, columns = tiles_ref.shape
    devices = len(gu_refs)
    width = down_refs[0].shape[0]
    chunks = row_chunks([[ref.shape[0] for ref in parts] for parts in gu_refs])
    copies = []
    for c, (first, length, sources) in enumerate(chunks):
        for d, (k, at) in enumerate(sources):
            copy = pltpu.make_async_copy(
                gu_refs[d][k].at[pl.ds(at, length)],
                gu_held.at[pl.ds(first, length), pl.ds(d * 2 * width, 2 * width)],
                gu_sem.at[c * devices + d],
            )
            copy.start()
            copies.append(copy)
    down_copies = []
    for d in range(devices):
        copy = pltpu.make_async_copy(
            down_refs[d], down_held.at[pl.ds(d * width, width)], down_sem.at[d]
        )
        copy.start()
        down_copies.append(copy)

    squares = 0.0
    for i in range(count):
        tile = tiles_ref[i].astype(jnp.float32)
        squares = squares + jnp.sum(tile * tile, axis=1, keepdims=True)
    scale = lax.rsqrt(squares / (count * columns) + 1e-05)
    logit = 0.0
    for i in range(count):
        span = slice(i * columns, (i + 1) * columns)
        tile = tiles_ref[i].astype(jnp.float32) * gain_ref[:, span] * scale
        x_ref[:, span] = tile.astype(jnp.bfloat16)
        rounded = x_ref[:, span].astype(jnp.float32)
        for e in range(EXPERTS):
            part = jnp.sum(rounded * router_ref[e : e + 1, span], axis=1, keepdims=True)
            logit = logit + part * sign_ref[:, e : e + 1]
    share = jax.nn.sigmoid(logit)

    for c, (first, length, _) in enumerate(chunks):
        for d in range(devices):
            copies[c * devices + d].wait()
        span = slice(first, first + length)
        piece = dot(x_ref[:, span], gu_held[span, :])
        both_ref[...] = piece if c == 0 else both_ref[...] + piece
    hidden = []
    for d in range(devices):
        gate = both_ref[:, 2 * d * width : (2 * d + 1) * width]
        up = both_ref[:, (2 * d + 1) * width : (2 * d + 2) * width]
        hidden.append((gate * jax.nn.sigmoid(gate) * up).astype(jnp.bfloat16))
    hidden = jnp.concatenate(hidden, axis=1)
    for copy in down_copies:
        copy.wait()
    for i in range(count):
        span = slice(i * columns, (i + 1) * columns)
        out_ref[i] = (dot(hidden, down_held[:, span]) * share).astype(out_ref.dtype)


def expert_call(out_shape, tiles, gain, router, sign, gate_ups, downs):
    vmem = pl.BlockSpec(memory_space=pltpu.VMEM)
    anywhere = pl.BlockSpec(memory_space=pl.ANY)
    rows, model = tiles.shape[1], tiles.shape[0] * tiles.shape[2]
    hidden = downs[0].shape[0]
    chunks = row_chunks([[g.shape[0] for g in parts] for parts in gate_ups])
    return pl.pallas_call(
        expert_kernel,
        out_shape=out_shape,
        in_specs=[vmem] * 4 + jax.tree.map(lambda _: anywhere, [gate_ups, downs]),
        out_specs=vmem,
        scratch_shapes=[
            pltpu.VMEM((rows, model), jnp.bfloat16),
            pltpu.VMEM((rows, len(downs) * 2 * hidden), jnp.float32),
            pltpu.VMEM((model, len(downs) * 2 * hidden), jnp.bfloat16),
            pltpu.VMEM((len(downs) * hidden, model), jnp.bfloat16),
            pltpu.SemaphoreType.DMA((len(chunks) * len(downs),)),
            pltpu.SemaphoreType.DMA((len(downs),)),
        ],
    )(tiles, gain, router, sign, gate_ups, downs)


def heads_of(spread_ref, i, rows, width, other):
    even = [spread_ref[i, :, j : j + rows] for j in range(0, width, CORES * rows)]
    odd = [spread_ref[i, :, j : j + rows] for j in range(rows, width, CORES * rows)]
    turn = (lax.axis_index("core") + other) % CORES == 0
    return jnp.where(turn, jnp.concatenate(even, axis=1), jnp.concatenate(odd, axis=1))


def project(spread_ref, proj_ref, rows, width, other):
    count = spread_ref.shape[0]
    depth = width // CORES
    total = None
    for i in range(count):
        piece = dot(
            heads_of(spread_ref, i, rows, width, other), proj_ref[i * depth : (i + 1) * depth, :]
        )
        total = piece if total is None else total + piece
    return total


def own_projection_kernel(rows, width, spread_ref, proj_ref, out_ref):
    out_ref[...] = project(spread_ref, proj_ref, rows, width, 0)


def other_projection_kernel(
    rows, width, spread_ref, proj_ref, before_ref, residual_ref, out_ref, copies_ref
):
    total = before_ref[...] + project(spread_ref, proj_ref, rows, width, 1)
    attended = (residual_ref[...].astype(jnp.float32) + total).astype(out_ref.dtype)
    out_ref[...] = attended
    for i in range(copies_ref.shape[0]):
        copies_ref[i] = attended


def in_vmem(kernel, out_shape, *operands):
    whole = pl.BlockSpec(memory_space=pltpu.VMEM)
    return pl.pallas_call(
        kernel,
        out_shape=out_shape,
        in_specs=jax.tree.map(lambda _: whole, operands),
        out_specs=jax.tree.map(lambda _: whole, out_shape),
    )(*operands)


def body(
    queries,
    keys_new,
    values_new,
    keys_past,
    values_past,
    block_order,
    residual,
    out_proj,
    norm_gain,
    router,
    w_gate,
    w_up,
    w_down,
    expert_ids,
):
    bf16, f32 = jnp.bfloat16, jnp.float32
    tok = queries.shape[0]
    head_dim = keys_new.shape[1]
    q_per = queries.shape[1] // head_dim
    width = queries.shape[1]
    past_len = keys_past.shape[0]
    rep_count = lax.axis_size("rep")
    scaling = 1.0 / math.sqrt(head_dim)

    count = lax.axis_size(CLASS)
    rows = count * tok
    kv_local = jnp.concatenate(
        [
            jnp.concatenate([keys_past, keys_new], axis=0),
            jnp.concatenate([values_past, values_new], axis=0),
        ],
        axis=1,
    )
    kv_pair = jnp.concatenate([kv_local, swapped(kv_local, "near")], axis=0)
    kv_all = jnp.concatenate([kv_pair, swapped(kv_pair, "core")], axis=0)
    out_proj_own = lax.all_gather(out_proj, ("far", "near"), axis=0, tiled=True)
    out_proj_other = swapped(out_proj_own, "core")

    model = w_gate.shape[1]
    cuts = [int(model * c) for c in CUTS]
    gate_up = jnp.concatenate([w_gate[0], w_up[0]], axis=1)
    down = w_down[0]
    gate_up_core = swapped(gate_up, "core")
    down_core = swapped(down, "core")
    zeroth_pair = swapped(gate_up[: cuts[0]], "near")
    zeroth_cross = swapped(zeroth_pair, "core")

    ids_wide = jnp.pad(expert_ids.astype(bf16), ((0, 0), (0, LANES - expert_ids.shape[1])))
    query_class = sent_to_all(jnp.concatenate([queries, ids_wide], axis=1), CLASS)
    query_class = query_class.reshape(rows, width + LANES)
    ids = query_class[:, width : width + 2].astype(jnp.int32)
    query_pos = (
        block_lookup(class_places(CLASS), block_order)[:, None] * tok
        + jnp.arange(tok, dtype=jnp.int32)[None, :]
    ).reshape(rows)

    key_span = past_len + tok
    key_owner_pos = block_lookup(jnp.stack(owners_by(SHARE)), block_order)
    offset = jnp.arange(key_span, dtype=jnp.int32) - past_len
    key_pos = jnp.where(
        offset[None, :] >= 0, key_owner_pos[:, None] * tok + offset[None, :], -1
    ).reshape(-1)
    visible = key_pos[None, :] <= query_pos[:, None]
    keys, values = kv_all[:, :head_dim], kv_all[:, head_dim:]
    heads = jnp.stack(
        [query_class[:, j * head_dim : (j + 1) * head_dim] for j in range(q_per)], axis=0
    )
    scores = jnp.einsum("jtd,kd->jtk", heads, keys, preferred_element_type=f32) * scaling
    scores = jnp.where(visible[None], scores, -1e30)
    shift = jnp.max(scores, axis=2).astype(bf16)
    weights = jnp.exp(scores - shift.astype(f32)[:, :, None])
    totals = jnp.sum(weights, axis=2)
    partial = jnp.einsum("jtk,kd->jtd", weights.astype(bf16), values, preferred_element_type=f32)
    totals_high = totals.astype(bf16)
    totals_low = (totals - totals_high.astype(f32)).astype(bf16)
    notes = jnp.concatenate([shift, totals_high, totals_low], axis=0).T
    notes = jnp.pad(notes, ((0, 0), (0, LANES - notes.shape[1])))
    message = jnp.concatenate([partial[j].astype(bf16) for j in range(q_per)] + [notes], axis=1)
    parts = exchanged(message.reshape(count, tok, width + LANES), CLASS)

    first_pair = swapped(after(gate_up[cuts[0] : cuts[1]], parts), "near")
    first_cross = swapped(first_pair, "core")
    part_shift = parts[:, :, width : width + q_per].astype(f32)
    part_total = parts[:, :, width + q_per : width + 2 * q_per].astype(f32) + parts[
        :, :, width + 2 * q_per : width + 3 * q_per
    ].astype(f32)
    level = jnp.exp(part_shift - jnp.max(part_shift, axis=0, keepdims=True))
    total = jnp.sum(level * part_total, axis=0)
    attn_local = jnp.concatenate(
        [
            jnp.sum(
                level[:, :, j : j + 1]
                * parts[:, :, j * head_dim : (j + 1) * head_dim].astype(f32),
                axis=0,
            )
            / total[:, j : j + 1]
            for j in range(q_per)
        ],
        axis=1,
    ).astype(bf16)

    spread = sent_to_all(jnp.concatenate([attn_local, keys_new, values_new], axis=1), "rep")
    keys_cache = side_by_side(spread[:, :, width : width + head_dim])
    values_cache = side_by_side(spread[:, :, width + head_dim :])
    shape = jax.ShapeDtypeStruct
    sizes = (out_proj.shape[0], width)
    own_part = in_vmem(
        functools.partial(own_projection_kernel, *sizes),
        shape(residual.shape, f32),
        spread,
        out_proj_own,
    )
    attended, attended_copies = in_vmem(
        functools.partial(other_projection_kernel, *sizes),
        (shape(residual.shape, bf16), shape((count, *residual.shape), bf16)),
        spread,
        out_proj_other,
        own_part,
        residual,
    )
    down_both = lax.all_gather(after(down, out_proj_own), "near", axis=0, tiled=True)
    down_pair = lax.dynamic_slice_in_dim(
        down_both, (1 - lax.axis_index("near")) * down.shape[0], down.shape[0]
    )
    down_cross = swapped(down_pair, "core")

    class_rows = rows
    class_width = attended.shape[1]
    class_attended = exchanged(attended_copies, CLASS).reshape(class_rows, class_width)
    second_pair = swapped(after(gate_up[cuts[1] :], class_attended), "near")
    second_cross = swapped(second_pair, "core")
    experts = jnp.arange(EXPERTS, dtype=jnp.int32)
    first_pick = (ids[:, 0:1] == experts[None, :]).astype(f32)
    second_pick = (ids[:, 1:2] == experts[None, :]).astype(f32)
    member = first_pick + second_pick
    row = jnp.arange(class_rows, dtype=jnp.int32)
    earlier = (row[:, None] // tok == row[None, :] // tok) & (row[None, :] < row[:, None])
    ranking = jnp.dot(
        earlier.astype(bf16), member.astype(bf16), preferred_element_type=f32
    ).astype(jnp.int32)
    slot_of = jnp.where(member > 0, (row[:, None] // tok) * CAP + ranking, -1)
    slot_count = count * CAP
    slots = jnp.arange(slot_count, dtype=jnp.int32)
    selection = (slot_of.T[:, None, :] == slots[None, :, None]).astype(bf16)
    halves = rep_count // EXPERTS
    back = jnp.concatenate([selection.reshape(EXPERTS * slot_count, class_rows)] * halves, axis=0)
    slot_rows = dot(back, class_attended).astype(bf16)
    arrived = exchanged(slot_rows.reshape(rep_count, slot_count, class_width), "rep")

    mine = lax.axis_index("rep") % EXPERTS
    my_selection = lax.dynamic_index_in_dim(selection, mine, axis=0, keepdims=False)
    slot_member = jnp.dot(my_selection, member.astype(bf16), preferred_element_type=f32)
    sign = jnp.where((experts == mine)[None, :], slot_member, -slot_member)
    outgoing = expert_call(
        shape((rep_count, slot_count, class_width), bf16),
        arrived,
        norm_gain[None, :],
        router.T,
        sign,
        [
            [gate_up],
            [gate_up_core],
            [zeroth_pair, first_pair, second_pair],
            [zeroth_cross, first_cross, second_cross],
        ],
        [down, down_core, down_pair, down_cross],
    )
    returned = exchanged(outgoing, "rep")

    mixture = lax.dot_general(
        back,
        returned.reshape(rep_count * slot_count, class_width),
        (((0,), (0,)), ((), ())),
        preferred_element_type=f32,
    ).astype(bf16)
    pieces = exchanged(mixture.reshape(count, tok, class_width), CLASS)
    layer_out = (attended.astype(f32) + jnp.sum(pieces.astype(f32), axis=0)).astype(bf16)
    return (attended, layer_out, keys_cache, values_cache)


def solution(mesh):
    far = mesh.shape["seq"] // (PAIR * CORES)
    split = Mesh(
        mesh.devices.reshape(mesh.shape["groups"], far, PAIR, CORES, mesh.shape["rep"]),
        ("groups", "far", "near", "core", "rep"),
    )
    return jax.shard_map(
        body,
        mesh=split,
        in_specs=(
            P(TOKENS, "rep"),
            P(TOKENS, "rep"),
            P(TOKENS, "rep"),
            P(TOKENS, "rep"),
            P(TOKENS, "rep"),
            P("groups"),
            P(TOKENS, "rep"),
            P(SEQ, "rep"),
            P(),
            P(),
            P("rep", None, SEQ),
            P("rep", None, SEQ),
            P("rep", SEQ, None),
            P(TOKENS, None),
        ),
        out_specs=(
            P(TOKENS, "rep"),
            P(TOKENS, "rep"),
            P(TOKENS, None),
            P(TOKENS, None),
        ),
        check_vma=False,
    )
```

```python
import functools
import math

import jax
import jax.numpy as jnp
from jax import lax
from jax.experimental import pallas as pl
from jax.experimental.pallas import tpu as pltpu
from jax.sharding import Mesh
from jax.sharding import PartitionSpec as P


EXPERTS = 4
CAP = 12
LANES = 128
PAIR = 2
CORES = 2
SEQ = ("far", "near", "core")
TOKENS = ("groups", "far", "near", "core")
SHARE = ("near", "core")
CLASS = ("far",)
CUTS = (9 / 32, 28 / 32)


def swapped(array, axis):
    return lax.ppermute(array, axis, [(0, 1), (1, 0)])


def after(array, ready):
    return lax.optimization_barrier((array, ready))[0]


def owners_by(axes):
    place = {a: lax.axis_index(a) for a in SEQ}
    held = [place]
    for axis in axes:
        held = held + [{**p, axis: 1 - p[axis]} for p in held]
    sizes = {a: lax.axis_size(a) for a in SEQ}
    return [(p["far"] * sizes["near"] + p["near"]) * sizes["core"] + p["core"] for p in held]


def exchanged(tiles, axis):
    return lax.all_to_all(tiles, axis, 0, 0, tiled=True)


def sent_to_all(array, axis):
    return exchanged(jnp.broadcast_to(array[None], (lax.axis_size(axis), *array.shape)), axis)


def side_by_side(tiles):
    return jnp.concatenate([tiles[i] for i in range(tiles.shape[0])], axis=1)


def block_lookup(owners, block_order):
    width = block_order.shape[0]
    hits = owners[:, None] == jnp.arange(width, dtype=jnp.int32)[None, :]
    return jnp.sum(jnp.where(hits, block_order[None, :], 0), axis=1)


def class_places(axes):
    sizes = {a: lax.axis_size(a) for a in SEQ}
    count = lax.axis_size(axes)
    index = jnp.arange(count, dtype=jnp.int32)
    place = {a: jnp.full((count,), lax.axis_index(a), jnp.int32) for a in SEQ}
    for axis in reversed(axes):
        place[axis] = index % sizes[axis]
        index = index // sizes[axis]
    return (place["far"] * sizes["near"] + place["near"]) * sizes["core"] + place["core"]


def dot(a, b):
    return jnp.dot(a, b, preferred_element_type=jnp.float32)


def row_chunks(parts_of_each):
    edges = {0}
    for parts in parts_of_each:
        at = 0
        for size in parts:
            edges.add(at + size)
            at += size
    edges = sorted(edges)
    fine = [edges[0]]
    for edge in edges[1:]:
        while edge - fine[-1] > 1280:
            fine.append(fine[-1] + 1024)
        fine.append(edge)
    chunks = []
    for first, last in zip(fine, fine[1:]):
        sources = []
        for parts in parts_of_each:
            at = 0
            for k, size in enumerate(parts):
                if at <= first < at + size:
                    sources.append((k, first - at))
                at += size
        chunks.append((first, last - first, sources))
    return chunks


def expert_kernel(
    tiles_ref,
    gain_ref,
    router_ref,
    sign_ref,
    gu_refs,
    down_refs,
    out_ref,
    x_ref,
    both_ref,
    gu_held,
    down_held,
    gu_sem,
    down_sem,
):
    count, _, columns = tiles_ref.shape
    devices = len(gu_refs)
    width = down_refs[0].shape[0]
    chunks = row_chunks([[ref.shape[0] for ref in parts] for parts in gu_refs])
    copies = []
    for c, (first, length, sources) in enumerate(chunks):
        for d, (k, at) in enumerate(sources):
            copy = pltpu.make_async_copy(
                gu_refs[d][k].at[pl.ds(at, length)],
                gu_held.at[pl.ds(first, length), pl.ds(d * 2 * width, 2 * width)],
                gu_sem.at[c * devices + d],
            )
            copy.start()
            copies.append(copy)
    down_copies = []
    for d in range(devices):
        copy = pltpu.make_async_copy(
            down_refs[d], down_held.at[pl.ds(d * width, width)], down_sem.at[d]
        )
        copy.start()
        down_copies.append(copy)

    squares, logit, done = 0.0, 0.0, 0
    for c, (first, length, _) in enumerate(chunks):
        while done * columns < first + length:
            span = slice(done * columns, (done + 1) * columns)
            tile = tiles_ref[done].astype(jnp.float32)
            squares = squares + jnp.sum(tile * tile, axis=1, keepdims=True)
            gained = tile * gain_ref[:, span]
            x_ref[:, span] = gained.astype(jnp.bfloat16)
            for e in range(EXPERTS):
                part = jnp.sum(gained * router_ref[e : e + 1, span], axis=1, keepdims=True)
                logit = logit + part * sign_ref[:, e : e + 1]
            done += 1
        for d in range(devices):
            copies[c * devices + d].wait()
        span = slice(first, first + length)
        piece = dot(x_ref[:, span], gu_held[span, :])
        both_ref[...] = piece if c == 0 else both_ref[...] + piece
    scale = lax.rsqrt(squares / (count * columns) + 1e-05)
    share = jax.nn.sigmoid(logit * scale)
    hidden = []
    for d in range(devices):
        gate = both_ref[:, 2 * d * width : (2 * d + 1) * width] * scale
        up = both_ref[:, (2 * d + 1) * width : (2 * d + 2) * width] * scale
        hidden.append((gate * jax.nn.sigmoid(gate) * up).astype(jnp.bfloat16))
    hidden = jnp.concatenate(hidden, axis=1)
    for copy in down_copies:
        copy.wait()
    for i in range(count):
        span = slice(i * columns, (i + 1) * columns)
        out_ref[i] = (dot(hidden, down_held[:, span]) * share).astype(out_ref.dtype)


def expert_call(out_shape, tiles, gain, router, sign, gate_ups, downs):
    vmem = pl.BlockSpec(memory_space=pltpu.VMEM)
    anywhere = pl.BlockSpec(memory_space=pl.ANY)
    rows, model = tiles.shape[1], tiles.shape[0] * tiles.shape[2]
    hidden = downs[0].shape[0]
    chunks = row_chunks([[g.shape[0] for g in parts] for parts in gate_ups])
    return pl.pallas_call(
        expert_kernel,
        out_shape=out_shape,
        in_specs=[vmem] * 4 + jax.tree.map(lambda _: anywhere, [gate_ups, downs]),
        out_specs=vmem,
        scratch_shapes=[
            pltpu.VMEM((rows, model), jnp.bfloat16),
            pltpu.VMEM((rows, len(downs) * 2 * hidden), jnp.float32),
            pltpu.VMEM((model, len(downs) * 2 * hidden), jnp.bfloat16),
            pltpu.VMEM((len(downs) * hidden, model), jnp.bfloat16),
            pltpu.SemaphoreType.DMA((len(chunks) * len(downs),)),
            pltpu.SemaphoreType.DMA((len(downs),)),
        ],
    )(tiles, gain, router, sign, gate_ups, downs)


def heads_of(spread_ref, i, rows, width, other):
    even = [spread_ref[i, :, j : j + rows] for j in range(0, width, CORES * rows)]
    odd = [spread_ref[i, :, j : j + rows] for j in range(rows, width, CORES * rows)]
    turn = (lax.axis_index("core") + other) % CORES == 0
    return jnp.where(turn, jnp.concatenate(even, axis=1), jnp.concatenate(odd, axis=1))


def project(spread_ref, proj_ref, rows, width, other):
    count = spread_ref.shape[0]
    depth = width // CORES
    total = None
    for i in range(count):
        piece = dot(
            heads_of(spread_ref, i, rows, width, other), proj_ref[i * depth : (i + 1) * depth, :]
        )
        total = piece if total is None else total + piece
    return total


def own_projection_kernel(rows, width, spread_ref, proj_ref, out_ref):
    out_ref[...] = project(spread_ref, proj_ref, rows, width, 0)


def other_projection_kernel(
    rows, width, spread_ref, proj_ref, before_ref, residual_ref, out_ref, copies_ref
):
    total = before_ref[...] + project(spread_ref, proj_ref, rows, width, 1)
    attended = (residual_ref[...].astype(jnp.float32) + total).astype(out_ref.dtype)
    out_ref[...] = attended
    for i in range(copies_ref.shape[0]):
        copies_ref[i] = attended


def in_vmem(kernel, out_shape, *operands):
    whole = pl.BlockSpec(memory_space=pltpu.VMEM)
    return pl.pallas_call(
        kernel,
        out_shape=out_shape,
        in_specs=jax.tree.map(lambda _: whole, operands),
        out_specs=jax.tree.map(lambda _: whole, out_shape),
    )(*operands)


def body(
    queries,
    keys_new,
    values_new,
    keys_past,
    values_past,
    block_order,
    residual,
    out_proj,
    norm_gain,
    router,
    w_gate,
    w_up,
    w_down,
    expert_ids,
):
    bf16, f32 = jnp.bfloat16, jnp.float32
    tok = queries.shape[0]
    head_dim = keys_new.shape[1]
    q_per = queries.shape[1] // head_dim
    width = queries.shape[1]
    past_len = keys_past.shape[0]
    rep_count = lax.axis_size("rep")
    scaling = 1.0 / math.sqrt(head_dim)

    count = lax.axis_size(CLASS)
    rows = count * tok
    kv_local = jnp.concatenate(
        [
            jnp.concatenate([keys_past, keys_new], axis=0),
            jnp.concatenate([values_past, values_new], axis=0),
        ],
        axis=1,
    )
    kv_pair = jnp.concatenate([kv_local, swapped(kv_local, "near")], axis=0)
    kv_all = jnp.concatenate([kv_pair, swapped(kv_pair, "core")], axis=0)
    out_proj_own = lax.all_gather(out_proj, ("far", "near"), axis=0, tiled=True)
    out_proj_other = swapped(out_proj_own, "core")

    model = w_gate.shape[1]
    cuts = [int(model * c) for c in CUTS]
    gate_up = jnp.concatenate([w_gate[0], w_up[0]], axis=1)
    down = w_down[0]
    gate_up_core = swapped(gate_up, "core")
    down_core = swapped(down, "core")
    zeroth_pair = swapped(gate_up[: cuts[0]], "near")
    zeroth_cross = swapped(zeroth_pair, "core")

    ids_wide = jnp.pad(expert_ids.astype(bf16), ((0, 0), (0, LANES - expert_ids.shape[1])))
    query_class = sent_to_all(jnp.concatenate([queries, ids_wide], axis=1), CLASS)
    query_class = query_class.reshape(rows, width + LANES)
    ids = query_class[:, width : width + 2].astype(jnp.int32)
    query_pos = (
        block_lookup(class_places(CLASS), block_order)[:, None] * tok
        + jnp.arange(tok, dtype=jnp.int32)[None, :]
    ).reshape(rows)

    key_span = past_len + tok
    key_owner_pos = block_lookup(jnp.stack(owners_by(SHARE)), block_order)
    offset = jnp.arange(key_span, dtype=jnp.int32) - past_len
    key_pos = jnp.where(
        offset[None, :] >= 0, key_owner_pos[:, None] * tok + offset[None, :], -1
    ).reshape(-1)
    visible = key_pos[None, :] <= query_pos[:, None]
    keys, values = kv_all[:, :head_dim], kv_all[:, head_dim:]
    heads = jnp.stack(
        [query_class[:, j * head_dim : (j + 1) * head_dim] for j in range(q_per)], axis=0
    )
    scores = jnp.einsum("jtd,kd->jtk", heads, keys, preferred_element_type=f32) * scaling
    scores = jnp.where(visible[None], scores, -1e30)
    shift = jnp.max(scores, axis=2).astype(bf16)
    weights = jnp.exp(scores - shift.astype(f32)[:, :, None])
    totals = jnp.sum(weights, axis=2)
    partial = jnp.einsum("jtk,kd->jtd", weights.astype(bf16), values, preferred_element_type=f32)
    totals_high = totals.astype(bf16)
    totals_low = (totals - totals_high.astype(f32)).astype(bf16)
    notes = jnp.concatenate([shift, totals_high, totals_low], axis=0).T
    notes = jnp.pad(notes, ((0, 0), (0, LANES - notes.shape[1])))
    message = jnp.concatenate([partial[j].astype(bf16) for j in range(q_per)] + [notes], axis=1)
    parts = exchanged(message.reshape(count, tok, width + LANES), CLASS)

    first_pair = swapped(after(gate_up[cuts[0] : cuts[1]], parts), "near")
    first_cross = swapped(first_pair, "core")
    part_shift = parts[:, :, width : width + q_per].astype(f32)
    part_total = parts[:, :, width + q_per : width + 2 * q_per].astype(f32) + parts[
        :, :, width + 2 * q_per : width + 3 * q_per
    ].astype(f32)
    level = jnp.exp(part_shift - jnp.max(part_shift, axis=0, keepdims=True))
    total = jnp.sum(level * part_total, axis=0)
    attn_local = jnp.concatenate(
        [
            jnp.sum(
                level[:, :, j : j + 1]
                * parts[:, :, j * head_dim : (j + 1) * head_dim].astype(f32),
                axis=0,
            )
            / total[:, j : j + 1]
            for j in range(q_per)
        ],
        axis=1,
    ).astype(bf16)

    spread = sent_to_all(jnp.concatenate([attn_local, keys_new, values_new], axis=1), "rep")
    keys_cache = side_by_side(spread[:, :, width : width + head_dim])
    values_cache = side_by_side(spread[:, :, width + head_dim :])
    shape = jax.ShapeDtypeStruct
    sizes = (out_proj.shape[0], width)
    own_part = in_vmem(
        functools.partial(own_projection_kernel, *sizes),
        shape(residual.shape, f32),
        spread,
        out_proj_own,
    )
    attended, attended_copies = in_vmem(
        functools.partial(other_projection_kernel, *sizes),
        (shape(residual.shape, bf16), shape((count, *residual.shape), bf16)),
        spread,
        out_proj_other,
        own_part,
        residual,
    )
    down_both = lax.all_gather(after(down, out_proj_own), "near", axis=0, tiled=True)
    down_pair = lax.dynamic_slice_in_dim(
        down_both, (1 - lax.axis_index("near")) * down.shape[0], down.shape[0]
    )
    down_cross = swapped(down_pair, "core")

    class_rows = rows
    class_width = attended.shape[1]
    class_attended = exchanged(attended_copies, CLASS).reshape(class_rows, class_width)
    second_pair = swapped(after(gate_up[cuts[1] :], class_attended), "near")
    second_cross = swapped(second_pair, "core")
    experts = jnp.arange(EXPERTS, dtype=jnp.int32)
    first_pick = (ids[:, 0:1] == experts[None, :]).astype(f32)
    second_pick = (ids[:, 1:2] == experts[None, :]).astype(f32)
    member = first_pick + second_pick
    row = jnp.arange(class_rows, dtype=jnp.int32)
    earlier = (row[:, None] // tok == row[None, :] // tok) & (row[None, :] < row[:, None])
    ranking = jnp.dot(
        earlier.astype(bf16), member.astype(bf16), preferred_element_type=f32
    ).astype(jnp.int32)
    slot_of = jnp.where(member > 0, (row[:, None] // tok) * CAP + ranking, -1)
    slot_count = count * CAP
    slots = jnp.arange(slot_count, dtype=jnp.int32)
    selection = (slot_of.T[:, None, :] == slots[None, :, None]).astype(bf16)
    halves = rep_count // EXPERTS
    back = jnp.concatenate([selection.reshape(EXPERTS * slot_count, class_rows)] * halves, axis=0)
    slot_rows = dot(back, class_attended).astype(bf16)
    arrived = exchanged(slot_rows.reshape(rep_count, slot_count, class_width), "rep")

    mine = lax.axis_index("rep") % EXPERTS
    my_selection = lax.dynamic_index_in_dim(selection, mine, axis=0, keepdims=False)
    slot_member = jnp.dot(my_selection, member.astype(bf16), preferred_element_type=f32)
    sign = jnp.where((experts == mine)[None, :], slot_member, -slot_member)
    outgoing = expert_call(
        shape((rep_count, slot_count, class_width), bf16),
        arrived,
        norm_gain[None, :],
        router.T,
        sign,
        [
            [gate_up],
            [gate_up_core],
            [zeroth_pair, first_pair, second_pair],
            [zeroth_cross, first_cross, second_cross],
        ],
        [down, down_core, down_pair, down_cross],
    )
    returned = exchanged(outgoing, "rep")

    mixture = lax.dot_general(
        back,
        returned.reshape(rep_count * slot_count, class_width),
        (((0,), (0,)), ((), ())),
        preferred_element_type=f32,
    ).astype(bf16)
    pieces = exchanged(mixture.reshape(count, tok, class_width), CLASS)
    layer_out = (attended.astype(f32) + jnp.sum(pieces.astype(f32), axis=0)).astype(bf16)
    return (attended, layer_out, keys_cache, values_cache)


def solution(mesh):
    far = mesh.shape["seq"] // (PAIR * CORES)
    split = Mesh(
        mesh.devices.reshape(mesh.shape["groups"], far, PAIR, CORES, mesh.shape["rep"]),
        ("groups", "far", "near", "core", "rep"),
    )
    return jax.shard_map(
        body,
        mesh=split,
        in_specs=(
            P(TOKENS, "rep"),
            P(TOKENS, "rep"),
            P(TOKENS, "rep"),
            P(TOKENS, "rep"),
            P(TOKENS, "rep"),
            P("groups"),
            P(TOKENS, "rep"),
            P(SEQ, "rep"),
            P(),
            P(),
            P("rep", None, SEQ),
            P("rep", None, SEQ),
            P("rep", SEQ, None),
            P(TOKENS, None),
        ),
        out_specs=(
            P(TOKENS, "rep"),
            P(TOKENS, "rep"),
            P(TOKENS, None),
            P(TOKENS, None),
        ),
        check_vma=False,
    )
```
